128 devices in a mesh: dp: 1, sub: 2 (over core), ep: 64 (over z, y, x).
Axes of the slice: x: 4, y: 4, z: 4, core: 2. Of those that a mesh axis runs over, the one named last changes fastest.
Arguments:
- x: bfloat16 [65536, 1024], P(('dp', 'sub', 'ep'))
- route_idx: int32 [65536, 2], P(('dp', 'sub', 'ep'))
- route_gate: float32 [65536, 2], P(('dp', 'sub', 'ep'))
- w_gate: bfloat16 [128, 1024, 512], P(('sub', 'ep'))
- w_up: bfloat16 [128, 1024, 512], P(('sub', 'ep'))
- w_down: bfloat16 [128, 512, 1024], P(('sub', 'ep'))
Outputs:
- output: bfloat16 [65536, 1024], P(('dp', 'sub', 'ep'))
All inputs are finite; a program needn't handle non-finite values.
Results may differ from the reference program's by a relative error of at most 0.001.
Values are sent between devices in bfloat16 or wider.
A program may use at most 1 GiB of HBM per device.

```python
import jax
import jax.numpy as jnp
from jax import lax

MODEL_DIM = 1024
EXPERT_FF = 512
EXPERTS = 128
TOK_DEV = 512
CAP_PAIR = 32


def draw_routes(rng_key, hot_id):
    k_wts, k_rank, k_swap, k_perm = jax.random.split(rng_key, 4)
    expert_ids = jnp.arange(EXPERTS, dtype=jnp.int32)
    is_hot = expert_ids == hot_id
    weights = jnp.where(is_hot, 0, jax.random.randint(k_wts, (EXPERTS,), 1, 3, dtype=jnp.int32))
    pool_size = 2 * TOK_DEV - CAP_PAIR - (EXPERTS - 1)
    shares = (pool_size * weights) // jnp.sum(weights)
    leftover = pool_size - jnp.sum(shares)
    rank_perm = jax.random.permutation(k_rank, EXPERTS)
    other_rank = rank_perm - (rank_perm > rank_perm[hot_id]).astype(jnp.int32)
    extra_one = ((other_rank < leftover) & jnp.logical_not(is_hot)).astype(jnp.int32)
    counts = jnp.where(is_hot, CAP_PAIR, 1 + shares + extra_one)
    bounds = jnp.cumsum(counts)
    slot_exp = jnp.searchsorted(bounds, jnp.arange(2 * TOK_DEV, dtype=jnp.int32), side='right').astype(jnp.int32)
    first_half = slot_exp[:TOK_DEV]
    second_half = slot_exp[TOK_DEV:]
    do_swap = jax.random.randint(k_swap, (TOK_DEV,), 0, 2, dtype=jnp.int32) == 1
    slot_pair = jnp.stack([jnp.where(do_swap, second_half, first_half), jnp.where(do_swap, first_half, second_half)], axis=1)
    return slot_pair[jax.random.permutation(k_perm, TOK_DEV)]


def setup_inputs(seed: int = 0, part: int = 0) -> dict:
    base_key = jax.random.key(seed)
    part_key = jax.random.fold_in(base_key, part)
    k_x, k_gate, k_hot, k_pick, k_route = jax.random.split(part_key, 5)
    k_w1, k_w3, k_w2 = jax.random.split(base_key, 3)
    tok_total = EXPERTS * TOK_DEV
    x = jax.random.normal(k_x, (tok_total, MODEL_DIM), jnp.float32).astype(jnp.bfloat16)
    hot_pair = jax.random.randint(k_hot, (2,), 0, EXPERTS, dtype=jnp.int32)
    hot_each = hot_pair[jax.random.randint(k_pick, (EXPERTS,), 0, 2, dtype=jnp.int32)]
    route_idx = jax.vmap(draw_routes)(jax.random.split(k_route, EXPERTS), hot_each).reshape(tok_total, 2)
    route_gate = jax.random.uniform(k_gate, (tok_total, 2), jnp.float32, 0.3, 0.7)
    w_gate = (jax.random.normal(k_w1, (EXPERTS, MODEL_DIM, EXPERT_FF), jnp.float32) * MODEL_DIM ** -0.5).astype(jnp.bfloat16)
    w_up = (jax.random.normal(k_w3, (EXPERTS, MODEL_DIM, EXPERT_FF), jnp.float32) * MODEL_DIM ** -0.5).astype(jnp.bfloat16)
    w_down = (jax.random.normal(k_w2, (EXPERTS, EXPERT_FF, MODEL_DIM), jnp.float32) * EXPERT_FF ** -0.5).astype(jnp.bfloat16)
    return {"x": x, "route_idx": route_idx, "route_gate": route_gate, "w_gate": w_gate, "w_up": w_up, "w_down": w_down}


def reference(x, route_idx, route_gate, w_gate, w_up, w_down):
    tok_total = x.shape[0]
    n_slots = 2 * tok_total
    buf_rows = EXPERTS * CAP_PAIR
    slot_exp = route_idx.reshape(n_slots)
    slot_gate = route_gate.reshape(n_slots)
    slot_order = jnp.argsort(slot_exp, stable=True)
    sorted_exp = slot_exp[slot_order]
    expert_ids = jnp.arange(EXPERTS, dtype=jnp.int32)
    run_start = jnp.searchsorted(sorted_exp, expert_ids, side='left')
    run_end = jnp.searchsorted(sorted_exp, expert_ids, side='right')
    offsets = jnp.arange(buf_rows, dtype=jnp.int32)

    def expert_step(y_acc, inputs):
        expert, w_gate_e, w_up_e, w_down_e = inputs
        slot_pos = run_start[expert] + offsets
        is_valid = slot_pos < run_end[expert]
        slot_sel = slot_order[jnp.minimum(slot_pos, n_slots - 1)]
        tok_sel = slot_sel // 2
        tok_rows = x[tok_sel]
        act_a = jnp.dot(tok_rows, w_gate_e, preferred_element_type=jnp.float32)
        act_b = jnp.dot(tok_rows, w_up_e, preferred_element_type=jnp.float32)
        hidden = (jax.nn.silu(act_a) * act_b).astype(jnp.bfloat16)
        out_rows = jnp.dot(hidden, w_down_e, preferred_element_type=jnp.float32).astype(jnp.bfloat16)
        weight = jnp.where(is_valid, slot_gate[slot_sel], 0.0)
        y_acc = y_acc.at[tok_sel].add(weight[:, None] * out_rows.astype(jnp.float32))
        return y_acc, None

    y_acc, _ = lax.scan(expert_step, jnp.zeros((tok_total, MODEL_DIM), jnp.float32), (expert_ids, w_gate, w_up, w_down))
    return y_acc.astype(jnp.bfloat16)
```

```python
import functools

import jax
import jax.numpy as jnp
from jax import lax
from jax.experimental import pallas as pl
from jax.experimental.pallas import tpu as pltpu
from jax.sharding import PartitionSpec as P

TILE = 256
VMEM_LIMIT = 56 * 1024 * 1024


def iota(shape, dim):
    return lax.broadcasted_iota(jnp.int32, shape, dim)


def ones_where(mask):
    return jnp.where(mask, 1.0, 0.0).astype(jnp.bfloat16)


def dot(a, b):
    return jnp.dot(a, b, preferred_element_type=jnp.float32)


def pack_kernel(cap, route_ref, x_ref, send_ref, pos_ref):
    tok = x_ref.shape[0]
    rows = send_ref.shape[0]
    lanes = iota((tok, rows // cap), 1)
    member0 = ones_where(route_ref[:, 0:1] == lanes)
    member1 = ones_where(route_ref[:, 1:2] == lanes)
    lower = ones_where(iota((tok, tok), 0) >= iota((tok, tok), 1))
    rank0 = dot(lower, member0)
    rank1 = dot(lower, member1) + rank0[tok - 1:tok, :]
    base = (lanes * cap - 1).astype(jnp.float32)
    pos0 = jnp.sum(jnp.where(member0 > 0, rank0 + base, 0.0), axis=1, keepdims=True)
    pos1 = jnp.sum(jnp.where(member1 > 0, rank1 + base, 0.0), axis=1, keepdims=True)
    pos_ref[...] = jnp.concatenate([pos0, pos1], axis=1).astype(jnp.int32)
    row0 = jnp.transpose(jnp.broadcast_to(pos0, (tok, 128)))[0:1, :]
    row1 = jnp.transpose(jnp.broadcast_to(pos1, (tok, 128)))[0:1, :]

    def block(i, carry):
        place = (iota((TILE, tok), 0) + i * TILE).astype(jnp.float32)
        pick = ones_where((place == row0) | (place == row1))
        send_ref[pl.ds(pl.multiple_of(i * TILE, TILE), TILE), :] = dot(pick, x_ref[...]).astype(jnp.bfloat16)
        return carry

    lax.fori_loop(0, rows // TILE, block, 0)


def ffn_kernel(x_ref, wg_ref, wu_ref, wd_ref, o_ref):
    rows = x_ref[...]
    act_a = dot(rows, wg_ref[...])
    act_b = dot(rows, wu_ref[...])
    hidden = (jax.nn.silu(act_a) * act_b).astype(jnp.bfloat16)
    o_ref[...] = dot(hidden, wd_ref[...]).astype(jnp.bfloat16)


def mix_kernel(ret_ref, pos_ref, gate_ref, y_ref):
    n_rows = ret_ref.shape[0]
    tok = y_ref.shape[0]
    for block in range(tok // TILE):
        part = pl.ds(block * TILE, TILE)
        lanes = iota((TILE, n_rows), 1)
        total = gate_ref[part, 0:1] * dot(ones_where(pos_ref[part, 0:1] == lanes), ret_ref[...])
        total = total + gate_ref[part, 1:2] * dot(ones_where(pos_ref[part, 1:2] == lanes), ret_ref[...])
        y_ref[part, :] = total.astype(jnp.bfloat16)


def solution(mesh):
    n_dev = mesh.shape["sub"] * mesh.shape["ep"]
    tok_spec = P(("dp", "sub", "ep"), None)
    expert_spec = P(("sub", "ep"), None, None)
    group = ("sub", "ep")
    vmem = pl.BlockSpec(memory_space=pltpu.VMEM)
    params = pltpu.CompilerParams(vmem_limit_bytes=VMEM_LIMIT)

    def device_step(x, route, gate, w_gate, w_up, w_down):
        tok, dim = x.shape
        ff = w_gate.shape[2]
        cap = min(tok, 8 * tok // n_dev)
        rows = n_dev * cap
        buffer = jax.ShapeDtypeStruct((rows, dim), jnp.bfloat16)
        send, pos = pl.pallas_call(
            functools.partial(pack_kernel, cap),
            out_shape=[buffer, jax.ShapeDtypeStruct((tok, 2), jnp.int32)],
            in_specs=[vmem, vmem],
            out_specs=[vmem, vmem],
            compiler_params=params,
            name="pack",
        )(route, x)
        got = lax.all_to_all(send.reshape(n_dev, cap, dim), group, 0, 0).reshape(rows, dim)
        out = pl.pallas_call(
            ffn_kernel,
            out_shape=buffer,
            grid=(rows // TILE,),
            in_specs=[
                pl.BlockSpec((TILE, dim), lambda i: (i, 0)),
                pl.BlockSpec((dim, ff), lambda i: (0, 0)),
                pl.BlockSpec((dim, ff), lambda i: (0, 0)),
                pl.BlockSpec((ff, dim), lambda i: (0, 0)),
            ],
            out_specs=pl.BlockSpec((TILE, dim), lambda i: (i, 0)),
            compiler_params=params,
            name="ffn",
        )(got, w_gate[0], w_up[0], w_down[0])
        ret = lax.all_to_all(out.reshape(n_dev, cap, dim), group, 0, 0).reshape(rows, dim)
        return pl.pallas_call(
            mix_kernel,
            out_shape=jax.ShapeDtypeStruct((tok, dim), jnp.bfloat16),
            in_specs=[vmem, vmem, vmem],
            out_specs=vmem,
            compiler_params=params,
            name="mix",
        )(ret, pos, gate)

    return jax.shard_map(
        device_step,
        mesh=mesh,
        in_specs=(tok_spec, tok_spec, tok_spec, expert_spec, expert_spec, expert_spec),
        out_specs=tok_spec,
        check_vma=False,
    )
```

```python
import functools

import jax
import jax.numpy as jnp
from jax import lax
from jax.experimental import pallas as pl
from jax.experimental.pallas import tpu as pltpu
from jax.sharding import PartitionSpec as P

MESH = pl.DeviceIdType.MESH
TILE = 256
VMEM_LIMIT = 60 * 1024 * 1024
COLORS = 3
PART = 4
BASE = COLORS * PART
SPARE = 8
OVER = COLORS * SPARE
SIDE = 4
TAIL = 128


def iota(shape, dim):
    return lax.broadcasted_iota(jnp.int32, shape, dim)


def ones_where(mask):
    return jnp.where(mask, 1.0, 0.0).astype(jnp.bfloat16)


def dot(a, b):
    return jnp.dot(a, b, preferred_element_type=jnp.float32)


def expert_ffn(rows, wg_ref, wu_ref, wd_ref):
    act_a = dot(rows, wg_ref[...])
    act_b = dot(rows, wu_ref[...])
    hidden = (jax.nn.silu(act_a) * act_b).astype(jnp.bfloat16)
    return dot(hidden, wd_ref[...]).astype(jnp.bfloat16)


def ranks(route_ref, n_experts):
    tok = route_ref.shape[0]
    lanes = iota((tok, n_experts), 1)
    member0 = route_ref[:, 0:1] == lanes
    member1 = route_ref[:, 1:2] == lanes
    lower = ones_where(iota((tok, tok), 0) >= iota((tok, tok), 1))
    rank0 = dot(lower, ones_where(member0))
    rank1 = dot(lower, ones_where(member1)) + rank0[tok - 1:tok, :]
    return member0, member1, rank0 - 1.0, rank1 - 1.0, rank1[tok - 1:tok, :]


def as_row(column):
    return jnp.transpose(jnp.broadcast_to(column, (column.shape[0], 128)))[0:1, :]


def wide_pack_kernel(cap, route_ref, x_ref, send_ref, pos_ref):
    tok = x_ref.shape[0]
    rows = send_ref.shape[0]
    member0, member1, rank0, rank1, _ = ranks(route_ref, rows // cap)
    base = (iota(member0.shape, 1) * cap).astype(jnp.float32)
    pos0 = jnp.sum(jnp.where(member0, rank0 + base, 0.0), axis=1, keepdims=True)
    pos1 = jnp.sum(jnp.where(member1, rank1 + base, 0.0), axis=1, keepdims=True)
    pos_ref[...] = jnp.concatenate([pos0, pos1], axis=1).astype(jnp.int32)
    row0, row1 = as_row(pos0), as_row(pos1)

    def block(i, carry):
        place = (iota((TILE, tok), 0) + i * TILE).astype(jnp.float32)
        pick = ones_where((place == row0) | (place == row1))
        send_ref[pl.ds(pl.multiple_of(i * TILE, TILE), TILE), :] = dot(pick, x_ref[...]).astype(jnp.bfloat16)
        return carry

    lax.fori_loop(0, rows // TILE, block, 0)


def wide_ffn_kernel(x_ref, wg_ref, wu_ref, wd_ref, o_ref):
    o_ref[...] = expert_ffn(x_ref[...], wg_ref, wu_ref, wd_ref)


def wide_mix_kernel(ret_ref, pos_ref, gate_ref, y_ref):
    n_rows = ret_ref.shape[0]

    def block(i, carry):
        part = pl.ds(pl.multiple_of(i * TILE, TILE), TILE)
        lanes = iota((TILE, n_rows), 1)
        total = gate_ref[part, 0:1] * dot(ones_where(pos_ref[part, 0:1] == lanes), ret_ref[...])
        total = total + gate_ref[part, 1:2] * dot(ones_where(pos_ref[part, 1:2] == lanes), ret_ref[...])
        y_ref[part, :] = total.astype(jnp.bfloat16)
        return carry

    lax.fori_loop(0, y_ref.shape[0] // TILE, block, 0)


def pack_kernel(route_ref, x_ref, send_ref, over_ref, pos_ref):
    tok, dim = x_ref.shape
    n_experts = send_ref.shape[1]
    rows = n_experts * PART
    member0, member1, rank0, rank1, count = ranks(route_ref, n_experts)
    lanes = iota((1, n_experts), 1)
    sub, ep = lanes // (SIDE ** 3), lanes % (SIDE ** 3)
    axes = (ep % SIDE, (ep // SIDE) % SIDE, ep // (SIDE * SIDE))
    first = []
    for color in range(COLORS):
        d1, d2, d3 = (axes[(color + i) % 3] for i in range(3))
        block = ((sub * SIDE + d1) * SIDE + d2) * SIDE + d3
        first.append((color * rows + block * PART - color * PART).astype(jnp.float32))
    excess = jnp.maximum(count - BASE, 0.0)
    strict = ones_where(iota((n_experts, n_experts), 0) < iota((n_experts, n_experts), 1))
    ahead = dot(jnp.broadcast_to(excess, (8, n_experts)).astype(jnp.bfloat16), strict)[0:1, :]
    total = jnp.sum(excess, axis=1, keepdims=True)
    nowhere = 4.0 * COLORS * rows

    def places(member, rank):
        base = jnp.where(rank < PART, first[0], jnp.where(rank < 2 * PART, first[1], first[2]))
        late = ahead + (rank - BASE)
        place = jnp.where(rank < BASE, base + rank, jnp.where(late < OVER, COLORS * rows + late, nowhere))
        return jnp.sum(jnp.where(member, place, 0.0), axis=1, keepdims=True)

    pos0, pos1 = places(member0, rank0), places(member1, rank1)
    pos_ref[...] = jnp.concatenate([pos0, pos1], axis=1).astype(jnp.int32)
    row0, row1 = as_row(pos0), as_row(pos1)

    def block(i, carry):
        place = (iota((TILE, tok), 0) + i * TILE).astype(jnp.float32)
        pick = ones_where((place == row0) | (place == row1))
        got = dot(pick, x_ref[...]).astype(jnp.bfloat16)
        half = rows // TILE
        send_ref[i // half, pl.ds((i % half) * (TILE // PART), TILE // PART)] = got.reshape(TILE // PART, PART, dim)
        return carry

    lax.fori_loop(0, COLORS * rows // TILE, block, 0)
    place = (iota((32, tok), 0) + COLORS * rows).astype(jnp.float32)
    pick0, pick1 = ones_where(place == row0), ones_where(place == row1)
    got = dot(pick0 + pick1, x_ref[...]).astype(jnp.bfloat16)
    expert0 = jnp.broadcast_to(route_ref[:, 0:1] + 1, (tok, TAIL)).astype(jnp.bfloat16)
    expert1 = jnp.broadcast_to(route_ref[:, 1:2] + 1, (tok, TAIL)).astype(jnp.bfloat16)
    owner = dot(pick0, expert0) + dot(pick1, expert1)
    flag = jnp.where(total > OVER, 1.0, 0.0)
    tail = jnp.where(iota((32, TAIL), 1) == 0, owner, flag).astype(jnp.bfloat16)
    for color in range(COLORS):
        part = slice(color * SPARE, (color + 1) * SPARE)
        over_ref[color, :, 0:dim] = got[part, :]
        over_ref[color, :, dim:dim + TAIL] = tail[part, :]


class Torus:
    def __init__(self):
        self.sub = lax.axis_index("sub")
        ep = lax.axis_index("ep")
        self.at = (ep % SIDE, (ep // SIDE) % SIDE, ep // (SIDE * SIDE))

    def coord(self, axis, step):
        return (self.at[axis] + step) % SIDE

    def device(self, axis, step, core=0):
        at = list(self.at)
        at[axis] = self.coord(axis, step)
        return {"sub": (self.sub + core) % 2, "ep": (at[2] * SIDE + at[1]) * SIDE + at[0]}

    def greet(self):
        barrier = pltpu.get_barrier_semaphore()
        peers = [self.device(0, 0, 1)]
        for axis in range(3):
            for step in range(1, SIDE):
                for core in range(2):
                    peers.append(self.device(axis, step, core))
        for peer in peers:
            pl.semaphore_signal(barrier, inc=1, device_id=peer, device_id_type=MESH)
        pl.semaphore_wait(barrier, len(peers))


def remote(src, dst, send_sem, recv_sem, device):
    copy = pltpu.make_async_remote_copy(
        src_ref=src, dst_ref=dst, send_sem=send_sem, recv_sem=recv_sem, device_id=device, device_id_type=MESH)
    copy.start()
    return copy


def local(src, dst, sem):
    copy = pltpu.make_async_copy(src, dst, sem)
    copy.start()
    return copy


def arrive(copies):
    for copy in copies:
        copy.wait_recv()


def settle(copies):
    for copy in copies:
        if copy.is_remote:
            copy.wait_send()


def out_kernel(a, over, d, every, b, c, send, recv, here, esend, erecv, ehere):
    t = Torus()
    t.greet()
    s = t.sub
    done = []

    def hop(phase, k):
        ax = (k + phase) % 3
        c1, c2, c3 = (t.at[(k + i) % 3] for i in range(3))
        copies = []
        if phase == 0:
            mine = every.at[s, k, c1, c2, c3]
            copies.append(local(over.at[k], mine, ehere.at[k]))
            for step in (1, 3, 2):
                copies.append(remote(over.at[k], mine, esend.at[phase, k, step], erecv.at[phase, k, step], t.device(ax, step)))
        elif phase == 1:
            part = every.at[s, k, :, c2, c3]
            for step in (1, 3, 2):
                copies.append(remote(part, part, esend.at[phase, k, step], erecv.at[phase, k, step], t.device(ax, step)))
        else:
            part = every.at[s, k, :, :, c3]
            for step in (1, 3, 2):
                copies.append(remote(part, part, esend.at[phase, k, step], erecv.at[phase, k, step], t.device(ax, step)))
        for step in (1, 3, 2, 0):
            to = t.coord(ax, step)
            if phase == 0:
                for core in range(2):
                    src, dst = a.at[k, (s + core) % 2, to], b.at[k, s, c1]
                    if step == 0 and core == 0:
                        copies.append(local(src, dst, here.at[phase, k]))
                    else:
                        copies.append(remote(src, dst, send.at[phase, k, 2 * step + core], recv.at[phase, k, 2 * step + core], t.device(ax, step, core)))
            else:
                src, dst = (b.at[k, :, :, to], c.at[k, c2]) if phase == 1 else (c.at[k, :, :, :, to], d.at[k, c3])
                if step == 0:
                    copies.append(local(src, dst, here.at[phase, k]))
                else:
                    copies.append(remote(src, dst, send.at[phase, k, 2 * step], recv.at[phase, k, 2 * step], t.device(ax, step)))
        done.extend(copies)
        return copies

    flight = [hop(0, k) for k in range(COLORS)]
    for phase in range(1, 3):
        for k in range(COLORS):
            arrive(flight[k])
            flight[k] = hop(phase, k)
    for k in range(COLORS):
        arrive(flight[k])
        part = every.at[s, k]
        flight[k] = [remote(part, part, esend.at[3, k, 0], erecv.at[3, k, 0], t.device(0, 0, 1))]
        done.extend(flight[k])
    for k in range(COLORS):
        arrive(flight[k])
    settle(done)


def back_kernel(d, every, a, over, b, c, stage, sum3, sum2, sum1, got3, got2, got1,
                send, recv, here, esend, erecv):
    t = Torus()
    t.greet()
    s = t.sub
    done = []

    def hop(phase, k):
        ax = (k + phase) % 3
        c1, c2, c3 = (t.at[(k + i) % 3] for i in range(3))
        copies = []
        for step in (1, 3, 2, 0):
            to = t.coord(ax, step)
            if phase == 0:
                for core in range(2):
                    src, dst = b.at[k, (s + core) % 2, to], a.at[k, s, c1]
                    if step == 0 and core == 0:
                        copies.append(local(src, dst, here.at[phase, k]))
                    else:
                        copies.append(remote(src, dst, send.at[phase, k, 2 * step + core], recv.at[phase, k, 2 * step + core], t.device(ax, step, core)))
            else:
                src, dst = (c.at[k, to], b.at[k, :, :, c2]) if phase == 1 else (d.at[k, to], c.at[k, :, :, :, c3])
                if step == 0:
                    copies.append(local(src, dst, here.at[phase, k]))
                else:
                    copies.append(remote(src, dst, send.at[phase, k, 2 * step], recv.at[phase, k, 2 * step], t.device(ax, step)))
        done.extend(copies)
        return copies

    def spread(phase, k):
        ax = (k + phase) % 3
        copies = []
        for step in (1, 3, 2):
            to = t.coord(ax, step)
            src = (sum1.at[k, to], sum2.at[k, :, to], sum3.at[k, :, :, to])[phase]
            dst = (got1, got2, got3)[phase].at[k, SIDE - step - 1]
            copies.append(remote(src, dst, esend.at[phase, k, step], erecv.at[phase, k, step], t.device(ax, step)))
        done.extend(copies)
        return copies

    def gather(phase, k):
        mine = t.at[(k + phase) % 3]
        got = (got1, got2, got3)[phase]
        more = got[k, 0] + got[k, 1] + got[k, 2]
        if phase == 2:
            sum2[k] = sum3[k, :, :, mine] + more
        elif phase == 1:
            sum1[k] = sum2[k, :, mine] + more
        else:
            over[k] = sum1[k, mine] + more

    swap = []
    for k in range(COLORS):
        swap.append([remote(every.at[1 - s, k], stage.at[k], esend.at[3, k, 0], erecv.at[3, k, 0], t.device(0, 0, 1))])
        done.extend(swap[k])
    flight = [hop(2, k) for k in range(COLORS)]
    extra = [None] * COLORS
    for k in range(COLORS):
        arrive(swap[k])

        def add(i, carry, k=k):
            sum3[k, i] = every[s, k, i] + stage[k, i]
            return carry

        lax.fori_loop(0, SIDE, add, 0)
    for k in range(COLORS):
        extra[k] = spread(2, k)
    for phase in (1, 0):
        for k in range(COLORS):
            arrive(flight[k])
            flight[k] = hop(phase, k)
        for k in range(COLORS):
            arrive(extra[k])
            gather(phase + 1, k)
        for k in range(COLORS):
            extra[k] = spread(phase, k)
    for k in range(COLORS):
        arrive(extra[k])
        gather(0, k)
    for k in range(COLORS):
        arrive(flight[k])
    settle(done)


def ffn_kernel(x_ref, wg_ref, wu_ref, wd_ref, o_ref):
    n, part, dim = x_ref.shape
    o_ref[...] = expert_ffn(x_ref[...].reshape(n * part, dim), wg_ref, wu_ref, wd_ref).reshape(n, part, dim)


def over_ffn_kernel(n_ep, x_ref, wg_ref, wu_ref, wd_ref, o_ref, flag_ref):
    n, part, width = x_ref.shape
    dim = o_ref.shape[2]
    me = (lax.axis_index("sub") * n_ep + lax.axis_index("ep") + 1).astype(jnp.float32)
    tail = x_ref[:, :, dim:width].reshape(n * part, width - dim).astype(jnp.float32)
    mine = tail[:, 0:1] == me

    @pl.when(pl.program_id(0) == 0)
    def _():
        flag_ref[...] = jnp.zeros_like(flag_ref)

    flag_ref[...] = jnp.maximum(flag_ref[...], jnp.max(tail[:, 1:2], axis=0, keepdims=True))
    any_mine = jnp.max(jnp.where(mine, 1.0, 0.0)) > 0.0

    @pl.when(any_mine)
    def _():
        rows = x_ref[:, :, 0:dim].reshape(n * part, dim)
        out = expert_ffn(rows, wg_ref, wu_ref, wd_ref)
        o_ref[...] = jnp.where(mine, out.astype(jnp.float32), 0.0).astype(jnp.bfloat16).reshape(n, part, dim)

    @pl.when(jnp.logical_not(any_mine))
    def _():
        o_ref[...] = jnp.zeros_like(o_ref)


def mix_kernel(main_ref, over_ref, pos_ref, gate_ref, y_ref, main, over):
    n, part, dim = main_ref.shape
    n_rows = n * part
    main[...] = main_ref[...].reshape(n_rows, dim)
    over[...] = jnp.zeros_like(over)
    for color in range(COLORS):
        over[color * SPARE:(color + 1) * SPARE, :] = over_ref[color]

    def block(i, carry):
        rows = pl.ds(pl.multiple_of(i * TILE, TILE), TILE)
        lanes = iota((TILE, n_rows), 1)
        more = iota((TILE, over.shape[0]), 1) + n_rows
        total = jnp.zeros((TILE, dim), jnp.float32)
        for slot in range(2):
            pos = pos_ref[rows, slot:slot + 1]
            got = dot(ones_where(pos == lanes), main[...]) + dot(ones_where(pos == more), over[...])
            total = total + gate_ref[rows, slot:slot + 1] * got
        y_ref[rows, :] = total.astype(jnp.bfloat16)
        return carry

    lax.fori_loop(0, y_ref.shape[0] // TILE, block, 0)


def solution(mesh):
    n_sub, n_ep = mesh.shape["sub"], mesh.shape["ep"]
    n_dev = n_sub * n_ep
    tok_spec = P(("dp", "sub", "ep"), None)
    expert_spec = P(("sub", "ep"), None, None)
    group = ("sub", "ep")
    vmem = pl.BlockSpec(memory_space=pltpu.VMEM)
    hbm = pl.BlockSpec(memory_space=pl.ANY)
    params = pltpu.CompilerParams(vmem_limit_bytes=VMEM_LIMIT)
    bf16 = jnp.bfloat16

    def shape(*dims):
        return jax.ShapeDtypeStruct(dims, bf16)

    def weights(dim, ff):
        return [
            pl.BlockSpec((dim, ff), lambda i: (0, 0)),
            pl.BlockSpec((dim, ff), lambda i: (0, 0)),
            pl.BlockSpec((ff, dim), lambda i: (0, 0)),
        ]

    def wide(x, route, gate, w_gate, w_up, w_down):
        tok, dim = x.shape
        ff = w_gate.shape[1]
        cap = min(tok, 8 * tok // n_dev)
        rows = n_dev * cap
        send, pos = pl.pallas_call(
            functools.partial(wide_pack_kernel, cap),
            out_shape=[shape(rows, dim), jax.ShapeDtypeStruct((tok, 2), jnp.int32)],
            in_specs=[vmem, vmem],
            out_specs=[vmem, vmem],
            compiler_params=params,
            name="wide_pack",
        )(route, x)
        got = lax.all_to_all(send.reshape(n_dev, cap, dim), group, 0, 0).reshape(rows, dim)
        block = pl.BlockSpec((TILE, dim), lambda i: (i, 0))
        out = pl.pallas_call(
            wide_ffn_kernel,
            out_shape=shape(rows, dim),
            grid=(rows // TILE,),
            in_specs=[block] + weights(dim, ff),
            out_specs=block,
            compiler_params=params,
            name="wide_ffn",
        )(got, w_gate, w_up, w_down)
        ret = lax.all_to_all(out.reshape(n_dev, cap, dim), group, 0, 0).reshape(rows, dim)
        return pl.pallas_call(
            wide_mix_kernel,
            out_shape=shape(tok, dim),
            in_specs=[vmem, vmem, vmem],
            out_specs=vmem,
            compiler_params=params,
            name="wide_mix",
        )(ret, pos, gate)

    def exchange_params(number):
        return pltpu.CompilerParams(collective_id=number, has_side_effects=True, vmem_limit_bytes=VMEM_LIMIT)

    cube = (SIDE, SIDE, SIDE)

    def device_step(x, route, gate, w_gate, w_up, w_down):
        tok, dim = x.shape
        ff = w_gate.shape[2]
        w_gate, w_up, w_down = w_gate[0], w_up[0], w_down[0]
        main = (COLORS, 2) + cube + (PART, dim)
        late = (2, COLORS) + cube + (SPARE, dim + TAIL)
        sems = pltpu.SemaphoreType.DMA
        send, over, pos = pl.pallas_call(
            pack_kernel,
            out_shape=[shape(COLORS, n_dev, PART, dim), shape(COLORS, SPARE, dim + TAIL),
                       jax.ShapeDtypeStruct((tok, 2), jnp.int32)],
            in_specs=[vmem, vmem],
            out_specs=[vmem, vmem, vmem],
            compiler_params=params,
            name="pack",
        )(route, x)
        got, late_in = pl.pallas_call(
            out_kernel,
            out_shape=[shape(COLORS, SIDE, SIDE, 2, SIDE, PART, dim), shape(*late)],
            in_specs=[vmem, vmem],
            out_specs=[vmem, vmem],
            scratch_shapes=[
                pltpu.VMEM((COLORS, 2, SIDE, SIDE, SIDE, PART, dim), bf16),
                pltpu.VMEM((COLORS, SIDE, 2, SIDE, SIDE, PART, dim), bf16),
                sems((3, COLORS, 2 * SIDE)), sems((3, COLORS, 2 * SIDE)), sems((3, COLORS)),
                sems((4, COLORS, SIDE)), sems((4, COLORS, SIDE)), sems((COLORS,)),
            ],
            compiler_params=exchange_params(0),
            name="exchange_out",
        )(send.reshape(main), over)
        blocks = COLORS * n_dev
        step = TILE // PART
        out = pl.pallas_call(
            ffn_kernel,
            out_shape=shape(blocks, PART, dim),
            grid=(blocks // step,),
            in_specs=[pl.BlockSpec((step, PART, dim), lambda i: (i, 0, 0))] + weights(dim, ff),
            out_specs=pl.BlockSpec((step, PART, dim), lambda i: (i, 0, 0)),
            compiler_params=params,
            name="ffn",
        )(got.reshape(blocks, PART, dim), w_gate, w_up, w_down)
        step = TILE // SPARE
        late_out, flag = pl.pallas_call(
            functools.partial(over_ffn_kernel, n_ep),
            out_shape=[shape(blocks, SPARE, dim), jax.ShapeDtypeStruct((1, 1), jnp.float32)],
            grid=(blocks // step,),
            in_specs=[pl.BlockSpec((step, SPARE, dim + TAIL), lambda i: (i, 0, 0))] + weights(dim, ff),
            out_specs=[pl.BlockSpec((step, SPARE, dim), lambda i: (i, 0, 0)), pl.BlockSpec((1, 1), lambda i: (0, 0))],
            compiler_params=params,
            name="over_ffn",
        )(late_in.reshape(blocks, SPARE, dim + TAIL), w_gate, w_up, w_down)
        ret, over_ret = pl.pallas_call(
            back_kernel,
            out_shape=[shape(*main), shape(COLORS, SPARE, dim)],
            in_specs=[vmem, vmem],
            out_specs=[vmem, vmem],
            scratch_shapes=[
                pltpu.VMEM((COLORS, 2, SIDE, SIDE, SIDE, PART, dim), bf16),
                pltpu.VMEM((COLORS, SIDE, 2, SIDE, SIDE, PART, dim), bf16),
                pltpu.VMEM((COLORS,) + cube + (SPARE, dim), bf16),
                pltpu.VMEM((COLORS,) + cube + (SPARE, dim), bf16),
                pltpu.VMEM((COLORS, SIDE, SIDE, SPARE, dim), bf16),
                pltpu.VMEM((COLORS, SIDE, SPARE, dim), bf16),
                pltpu.VMEM((COLORS, SIDE - 1, SIDE, SIDE, SPARE, dim), bf16),
                pltpu.VMEM((COLORS, SIDE - 1, SIDE, SPARE, dim), bf16),
                pltpu.VMEM((COLORS, SIDE - 1, SPARE, dim), bf16),
                sems((3, COLORS, 2 * SIDE)), sems((3, COLORS, 2 * SIDE)), sems((3, COLORS)),
                sems((4, COLORS, SIDE)), sems((4, COLORS, SIDE)),
            ],
            compiler_params=exchange_params(1),
            name="exchange_back",
        )(out.reshape((COLORS, SIDE, SIDE, 2, SIDE, PART, dim)), late_out.reshape(late[:-1] + (dim,)))
        y = pl.pallas_call(
            mix_kernel,
            out_shape=shape(tok, dim),
            in_specs=[vmem] * 4,
            out_specs=vmem,
            scratch_shapes=[pltpu.VMEM((blocks * PART, dim), bf16), pltpu.VMEM((128, dim), bf16)],
            compiler_params=params,
            name="mix",
        )(ret.reshape(blocks, PART, dim), over_ret, pos, gate)
        return lax.cond(flag[0, 0] > 0.0, wide, lambda *args: y, x, route, gate, w_gate, w_up, w_down)

    return jax.shard_map(
        device_step,
        mesh=mesh,
        in_specs=(tok_spec, tok_spec, tok_spec, expert_spec, expert_spec, expert_spec),
        out_specs=tok_spec,
        check_vma=False,
    )
```

```python
import functools

import jax
import jax.numpy as jnp
from jax import lax
from jax.experimental import pallas as pl
from jax.experimental.pallas import tpu as pltpu
from jax.sharding import PartitionSpec as P

MESH = pl.DeviceIdType.MESH
TILE = 256
VMEM_LIMIT = 60 * 1024 * 1024
COLORS = 3
PART = 4
BASE = COLORS * PART
SPARE = 8
OVER = COLORS * SPARE
SIDE = 4
TAIL = 128


def iota(shape, dim):
    return lax.broadcasted_iota(jnp.int32, shape, dim)


def ones_where(mask):
    return jnp.where(mask, 1.0, 0.0).astype(jnp.bfloat16)


def dot(a, b):
    return jnp.dot(a, b, preferred_element_type=jnp.float32)


def expert_ffn(rows, wg_ref, wu_ref, wd_ref):
    act_a = dot(rows, wg_ref[...])
    act_b = dot(rows, wu_ref[...])
    hidden = (jax.nn.silu(act_a) * act_b).astype(jnp.bfloat16)
    return dot(hidden, wd_ref[...]).astype(jnp.bfloat16)


def ranks(route_ref, n_experts):
    tok = route_ref.shape[0]
    lanes = iota((tok, n_experts), 1)
    member0 = route_ref[:, 0:1] == lanes
    member1 = route_ref[:, 1:2] == lanes
    lower = ones_where(iota((tok, tok), 0) >= iota((tok, tok), 1))
    rank0 = dot(lower, ones_where(member0))
    rank1 = dot(lower, ones_where(member1)) + rank0[tok - 1:tok, :]
    return member0, member1, rank0 - 1.0, rank1 - 1.0, rank1[tok - 1:tok, :]


def as_row(column):
    return jnp.transpose(jnp.broadcast_to(column, (column.shape[0], 128)))[0:1, :]


def wide_pack_kernel(cap, route_ref, x_ref, send_ref, pos_ref):
    tok = x_ref.shape[0]
    rows = send_ref.shape[0]
    member0, member1, rank0, rank1, _ = ranks(route_ref, rows // cap)
    base = (iota(member0.shape, 1) * cap).astype(jnp.float32)
    pos0 = jnp.sum(jnp.where(member0, rank0 + base, 0.0), axis=1, keepdims=True)
    pos1 = jnp.sum(jnp.where(member1, rank1 + base, 0.0), axis=1, keepdims=True)
    pos_ref[...] = jnp.concatenate([pos0, pos1], axis=1).astype(jnp.int32)
    row0, row1 = as_row(pos0), as_row(pos1)

    def block(i, carry):
        place = (iota((TILE, tok), 0) + i * TILE).astype(jnp.float32)
        pick = ones_where((place == row0) | (place == row1))
        send_ref[pl.ds(pl.multiple_of(i * TILE, TILE), TILE), :] = dot(pick, x_ref[...]).astype(jnp.bfloat16)
        return carry

    lax.fori_loop(0, rows // TILE, block, 0)


def wide_ffn_kernel(x_ref, wg_ref, wu_ref, wd_ref, o_ref):
    o_ref[...] = expert_ffn(x_ref[...], wg_ref, wu_ref, wd_ref)


def wide_mix_kernel(ret_ref, pos_ref, gate_ref, y_ref):
    n_rows = ret_ref.shape[0]

    def block(i, carry):
        part = pl.ds(pl.multiple_of(i * TILE, TILE), TILE)
        lanes = iota((TILE, n_rows), 1)
        total = gate_ref[part, 0:1] * dot(ones_where(pos_ref[part, 0:1] == lanes), ret_ref[...])
        total = total + gate_ref[part, 1:2] * dot(ones_where(pos_ref[part, 1:2] == lanes), ret_ref[...])
        y_ref[part, :] = total.astype(jnp.bfloat16)
        return carry

    lax.fori_loop(0, y_ref.shape[0] // TILE, block, 0)


class Torus:
    def __init__(self):
        self.sub = lax.axis_index("sub")
        ep = lax.axis_index("ep")
        self.at = (ep % SIDE, (ep // SIDE) % SIDE, ep // (SIDE * SIDE))

    def coord(self, axis, step):
        return (self.at[axis] + step) % SIDE

    def device(self, axis, step, core=0):
        at = list(self.at)
        at[axis] = self.coord(axis, step)
        return {"sub": (self.sub + core) % 2, "ep": (at[2] * SIDE + at[1]) * SIDE + at[0]}

    def greet(self):
        barrier = pltpu.get_barrier_semaphore()
        peers = [self.device(0, 0, 1)]
        for axis in range(3):
            for step in range(1, SIDE):
                for core in range(2):
                    peers.append(self.device(axis, step, core))
        for peer in peers:
            pl.semaphore_signal(barrier, inc=1, device_id=peer, device_id_type=MESH)
        pl.semaphore_wait(barrier, len(peers))


def remote(src, dst, send_sem, recv_sem, device):
    return pltpu.make_async_remote_copy(
        src_ref=src, dst_ref=dst, send_sem=send_sem, recv_sem=recv_sem, device_id=device, device_id_type=MESH)


def start(copies):
    for copy in copies:
        copy.start()


def arrive(copies):
    for copy in copies:
        copy.wait_recv()


def settle(copies):
    for copy in copies:
        if copy.is_remote:
            copy.wait_send()


def at(i, table):
    for j, steps in table.items():
        @pl.when(i == j)
        def _(steps=steps):
            for step in steps:
                step()


STEPS = (1, 3, 2)
CHUNKS = [(k, h) for h in range(2) for k in range(COLORS)]


def layer_kernel(route_ref, gate_ref, x_ref, wg_hbm, wu_hbm, wd_hbm, y_ref, flag_ref,
                 wg, wu, wd, a, b, c, d, cc, bb, aa, over, every, late, stage, sum2, sum1, got3, got2, got1, last,
                 pos, total, send, recv, bsend, brecv, esend, erecv, rsend, rrecv, here, wsem):
    tok, dim = x_ref.shape
    rows = 2 * SIDE ** 3 * PART
    t = Torus()
    s = t.sub
    load = [pltpu.make_async_copy(src, dst, wsem.at[i])
            for i, (src, dst) in enumerate(((wg_hbm, wg), (wu_hbm, wu), (wd_hbm, wd)))]
    start(load)
    t.greet()

    def place(k):
        return tuple(t.at[(k + i) % 3] for i in range(3))

    def out(phase, k, h):
        ax, sh = (k + phase) % 3, (s + h) % 2
        c1, c2, c3 = place(k)
        copies = []
        for step in STEPS + (0,):
            to = t.coord(ax, step)
            core = h if phase == 0 else 0
            if phase == 0:
                src, dst = a.at[k, sh, to], b.at[k, s, c1]
            elif phase == 1:
                src, dst = b.at[k, sh, :, to], c.at[k, sh, c2]
            else:
                src, dst = c.at[k, sh, :, :, to], d.at[k, sh, c3]
            if step == 0 and core == 0:
                copies.append(pltpu.make_async_copy(src, dst, recv.at[phase, k, h, step]))
            else:
                copies.append(remote(src, dst, send.at[phase, k, h, step], recv.at[phase, k, h, step],
                                     t.device(ax, step, core)))
        return copies

    def back(phase, k, h):
        ax, sh = (k + phase) % 3, (s + h) % 2
        c1, c2, c3 = place(k)
        copies = []
        for step in STEPS + (0,):
            to = t.coord(ax, step)
            core = h if phase == 0 else 0
            if phase == 0:
                src, dst = bb.at[k, sh, to], aa.at[k, s, c1]
            elif phase == 1:
                src, dst = cc.at[k, sh, to], bb.at[k, sh, :, c2]
            else:
                src, dst = d.at[k, sh, to], cc.at[k, sh, :, :, c3]
            if step == 0 and core == 0:
                copies.append(pltpu.make_async_copy(src, dst, brecv.at[phase, k, h, step]))
            else:
                copies.append(remote(src, dst, bsend.at[phase, k, h, step], brecv.at[phase, k, h, step],
                                     t.device(ax, step, core)))
        return copies

    def gather(phase, k):
        c1, c2, c3 = place(k)
        if phase == 3:
            part = every.at[s, k]
            return [remote(part, part, esend.at[3, k, 0], erecv.at[3, k, 0], t.device(0, 0, 1))]
        mine = (every.at[s, k, c1, c2, c3], every.at[s, k, :, c2, c3], every.at[s, k, :, :, c3])[phase]
        copies = [remote(mine, mine, esend.at[phase, k, step], erecv.at[phase, k, step],
                         t.device((k + phase) % 3, step)) for step in STEPS]
        return copies

    def reduce(phase, k):
        if phase == 3:
            return [remote(late.at[1 - s, k], stage.at[k], rsend.at[3, k, 0], rrecv.at[3, k, 0], t.device(0, 0, 1))]
        copies = []
        for step in STEPS:
            to = t.coord((k + phase) % 3, step)
            src = (sum1.at[k, to], sum2.at[k, :, to], late.at[s, k, :, :, to])[phase]
            dst = (got1, got2, got3)[phase].at[k, SIDE - step - 1]
            copies.append(remote(src, dst, rsend.at[phase, k, step], rrecv.at[phase, k, step],
                                 t.device((k + phase) % 3, step)))
        return copies

    def merge(phase, k):
        if phase == 3:
            def add(i, carry):
                late[s, k, i] = late[s, k, i] + stage[k, i]
                return carry

            lax.fori_loop(0, SIDE, add, 0)
            return
        mine = t.at[(k + phase) % 3]
        got = (got1, got2, got3)[phase]
        more = got[k, 0] + got[k, 1] + got[k, 2]
        if phase == 2:
            sum2[k] = late[s, k, :, :, mine] + more
        elif phase == 1:
            sum1[k] = sum2[k, :, mine] + more
        else:
            last[k * SPARE:(k + 1) * SPARE, :] = sum1[k, mine] + more

    n_experts = 2 * SIDE ** 3
    member0, member1, rank0, rank1, count = ranks(route_ref, n_experts)
    lanes = iota((1, n_experts), 1)
    sub, ep = lanes // (SIDE ** 3), lanes % (SIDE ** 3)
    axes = (ep % SIDE, (ep // SIDE) % SIDE, ep // (SIDE * SIDE))
    first = []
    for k in range(COLORS):
        d1, d2, d3 = (axes[(k + i) % 3] for i in range(3))
        block = ((sub * SIDE + d1) * SIDE + d2) * SIDE + d3
        first.append((k * rows + block * PART - k * PART).astype(jnp.float32))
    excess = jnp.maximum(count - BASE, 0.0)
    strict = ones_where(iota((n_experts, n_experts), 0) < iota((n_experts, n_experts), 1))
    ahead = dot(jnp.broadcast_to(excess, (8, n_experts)).astype(jnp.bfloat16), strict)[0:1, :]
    n_over = jnp.sum(excess, axis=1, keepdims=True)
    nowhere = 4.0 * COLORS * rows

    def places(member, rank):
        base = jnp.where(rank < PART, first[0], jnp.where(rank < 2 * PART, first[1], first[2]))
        behind = ahead + (rank - BASE)
        where = jnp.where(rank < BASE, base + rank, jnp.where(behind < OVER, COLORS * rows + behind, nowhere))
        return jnp.sum(jnp.where(member, where, 0.0), axis=1, keepdims=True)

    pos0, pos1 = places(member0, rank0), places(member1, rank1)
    pos[:, 0:1] = pos0.astype(jnp.int32)
    pos[:, 1:2] = pos1.astype(jnp.int32)
    row0, row1 = as_row(pos0), as_row(pos1)

    spot = (iota((32, tok), 0) + COLORS * rows).astype(jnp.float32)
    pick0, pick1 = ones_where(spot == row0), ones_where(spot == row1)
    got = dot(pick0 + pick1, x_ref[...]).astype(jnp.bfloat16)
    expert0 = jnp.broadcast_to(route_ref[:, 0:1] + 1, (tok, TAIL)).astype(jnp.bfloat16)
    expert1 = jnp.broadcast_to(route_ref[:, 1:2] + 1, (tok, TAIL)).astype(jnp.bfloat16)
    owner = dot(pick0, expert0) + dot(pick1, expert1)
    flag = jnp.where(n_over > OVER, 1.0, 0.0)
    tail = jnp.where(iota((32, TAIL), 1) == 0, owner, flag).astype(jnp.bfloat16)
    for k in range(COLORS):
        c1, c2, c3 = place(k)
        part = slice(k * SPARE, (k + 1) * SPARE)
        every[s, k, c1, c2, c3, :, 0:dim] = got[part, :]
        every[s, k, c1, c2, c3, :, dim:dim + TAIL] = tail[part, :]

    half = rows // TILE

    def pack(i, carry):
        spot = (iota((TILE, tok), 0) + i * TILE).astype(jnp.float32)
        pick = ones_where((spot == row0) | (spot == row1))
        got = dot(pick, x_ref[...]).astype(jnp.bfloat16)
        a[i // half, i % half] = got.reshape(SIDE, SIDE, SIDE, PART, dim)
        at(i, {
            2: [lambda: start(out(0, 0, 0)), lambda: start(out(0, 0, 1))],
            4: [lambda: start(out(0, 1, 0)), lambda: start(out(0, 1, 1))],
        })
        return carry

    lax.fori_loop(0, COLORS * half, pack, 0)
    start(out(0, 2, 0) + out(0, 2, 1))
    for k in range(COLORS):
        start(gather(0, k))
    for phase in range(1, 3):
        for k, h in CHUNKS:
            arrive(out(phase - 1, k, h))
            start(out(phase, k, h))
        for k in range(COLORS):
            arrive(gather(phase - 1, k))
            start(gather(phase, k))
    arrive(load)

    def ffn(i, carry):
        k, h = i % COLORS, i // COLORS
        sh = (s + h) % 2
        at(i, {j: [lambda q=q: arrive(out(2, *q))] for j, q in enumerate(CHUNKS)})
        d[k, sh] = expert_ffn(d[k, sh].reshape(TILE, dim), wg, wu, wd).reshape(SIDE, SIDE, SIDE, PART, dim)
        at(i, {j: [lambda q=q: start(back(2, *q))] for j, q in enumerate(CHUNKS)})
        return carry

    lax.fori_loop(0, len(CHUNKS), ffn, 0)

    me = (s * SIDE ** 3 + lax.axis_index("ep") + 1).astype(jnp.float32)
    flag_ref[...] = jnp.zeros_like(flag_ref)
    order = [2, 4, 5, 7, 9, 10]

    def over_ffn(i, carry):
        core, k, part = (s + i // 6) % 2, (i // 2) % COLORS, (i % 2) * 2
        before = {j: [lambda j=j: arrive(gather(2, j)), lambda j=j: start(gather(3, j))] for j in range(COLORS)}
        before.update({6 + 2 * j: [lambda j=j: arrive(gather(3, j))] for j in range(COLORS)})
        at(i, before)
        got = every[core, k, pl.ds(part, 2)].reshape(TILE, dim + TAIL)
        tail = got[:, dim:dim + TAIL].astype(jnp.float32)
        flag_ref[...] = jnp.maximum(flag_ref[...], jnp.max(tail[:, 1:2], axis=0, keepdims=True))
        result = expert_ffn(got[:, 0:dim], wg, wu, wd).astype(jnp.float32)
        result = jnp.where(tail[:, 0:1] == me, result, 0.0).astype(jnp.bfloat16)
        late[core, k, pl.ds(part, 2)] = result.reshape(2, SIDE, SIDE, SPARE, dim)
        at(i, {order[j]: [lambda q=q: arrive(back(2, *q)), lambda q=q: start(back(1, *q))]
               for j, q in enumerate(CHUNKS)})
        at(i, {8: [lambda: start(reduce(3, 0))]})
        return carry

    lax.fori_loop(0, 12, over_ffn, 0)
    start(reduce(3, 1))
    start(reduce(3, 2))
    for k in range(COLORS):
        arrive(reduce(3, k))
        merge(3, k)
        if k:
            start(reduce(2, k - 1))
    start(reduce(2, 2))
    for k, h in CHUNKS:
        arrive(back(1, k, h))
        start(back(0, k, h))
    for phase in (2, 1):
        for k in range(COLORS):
            arrive(reduce(phase, k))
            merge(phase, k)
            if k:
                start(reduce(phase - 1, k - 1))
        start(reduce(phase - 1, 2))
    total[...] = jnp.zeros_like(total)

    def mix(i, carry):
        at(i, {k: [lambda k=k: arrive(back(0, k, 0)), lambda k=k: arrive(back(0, k, 1))] for k in range(COLORS)})
        got = aa[i].reshape(rows, dim)
        lanes = iota((TILE, rows), 1) + i * rows
        for part in range(tok // TILE):
            where = pl.ds(part * TILE, TILE)
            for slot in range(2):
                pick = ones_where(pos[where, slot:slot + 1] == lanes)
                total[where, :] += gate_ref[where, slot:slot + 1] * dot(pick, got)
        return carry

    lax.fori_loop(0, COLORS, mix, 0)
    last[...] = jnp.zeros_like(last)
    for k in range(COLORS):
        arrive(reduce(0, k))
        merge(0, k)
    lanes = iota((tok, last.shape[0]), 1) + COLORS * rows
    more = jnp.zeros((tok, dim), jnp.float32)
    for slot in range(2):
        more = more + gate_ref[:, slot:slot + 1] * dot(ones_where(pos[:, slot:slot + 1] == lanes), last[...])
    y_ref[...] = (total[...] + more).astype(jnp.bfloat16)
    for k in range(COLORS):
        for phase in range(3):
            for h in range(2):
                settle(out(phase, k, h) + back(phase, k, h))
        for phase in range(4):
            settle(gather(phase, k) + reduce(phase, k))


def solution(mesh):
    n_sub, n_ep = mesh.shape["sub"], mesh.shape["ep"]
    n_dev = n_sub * n_ep
    tok_spec = P(("dp", "sub", "ep"), None)
    expert_spec = P(("sub", "ep"), None, None)
    group = ("sub", "ep")
    vmem = pl.BlockSpec(memory_space=pltpu.VMEM)
    hbm = pl.BlockSpec(memory_space=pl.ANY)
    params = pltpu.CompilerParams(vmem_limit_bytes=VMEM_LIMIT)
    bf16 = jnp.bfloat16

    def shape(*dims):
        return jax.ShapeDtypeStruct(dims, bf16)

    def weights(dim, ff):
        return [
            pl.BlockSpec((dim, ff), lambda i: (0, 0)),
            pl.BlockSpec((dim, ff), lambda i: (0, 0)),
            pl.BlockSpec((ff, dim), lambda i: (0, 0)),
        ]

    def wide(x, route, gate, w_gate, w_up, w_down):
        tok, dim = x.shape
        ff = w_gate.shape[1]
        cap = min(tok, 8 * tok // n_dev)
        rows = n_dev * cap
        send, pos = pl.pallas_call(
            functools.partial(wide_pack_kernel, cap),
            out_shape=[shape(rows, dim), jax.ShapeDtypeStruct((tok, 2), jnp.int32)],
            in_specs=[vmem, vmem],
            out_specs=[vmem, vmem],
            compiler_params=params,
            name="wide_pack",
        )(route, x)
        got = lax.all_to_all(send.reshape(n_dev, cap, dim), group, 0, 0).reshape(rows, dim)
        block = pl.BlockSpec((TILE, dim), lambda i: (i, 0))
        out = pl.pallas_call(
            wide_ffn_kernel,
            out_shape=shape(rows, dim),
            grid=(rows // TILE,),
            in_specs=[block] + weights(dim, ff),
            out_specs=block,
            compiler_params=params,
            name="wide_ffn",
        )(got, w_gate, w_up, w_down)
        ret = lax.all_to_all(out.reshape(n_dev, cap, dim), group, 0, 0).reshape(rows, dim)
        return pl.pallas_call(
            wide_mix_kernel,
            out_shape=shape(tok, dim),
            in_specs=[vmem, vmem, vmem],
            out_specs=vmem,
            compiler_params=params,
            name="wide_mix",
        )(ret, pos, gate)

    cube = (SIDE, SIDE, SIDE)

    def device_step(x, route, gate, w_gate, w_up, w_down):
        tok, dim = x.shape
        ff = w_gate.shape[2]
        w_gate, w_up, w_down = w_gate[0], w_up[0], w_down[0]
        sems = pltpu.SemaphoreType.DMA
        main = pltpu.VMEM((COLORS, 2) + cube + (PART, dim), bf16)
        pairs = sems((3, COLORS, 2, SIDE))
        quads = sems((4, COLORS, SIDE))
        y, flag = pl.pallas_call(
            layer_kernel,
            out_shape=[shape(tok, dim), jax.ShapeDtypeStruct((1, 1), jnp.float32)],
            in_specs=[vmem, vmem, vmem, hbm, hbm, hbm],
            out_specs=[vmem, vmem],
            scratch_shapes=[
                pltpu.VMEM((dim, ff), bf16), pltpu.VMEM((dim, ff), bf16), pltpu.VMEM((ff, dim), bf16),
                main, main, main, main, main, main, main,
                pltpu.VMEM((COLORS, SPARE, dim + TAIL), bf16),
                pltpu.VMEM((2, COLORS) + cube + (SPARE, dim + TAIL), bf16),
                pltpu.VMEM((2, COLORS) + cube + (SPARE, dim), bf16),
                pltpu.VMEM((COLORS,) + cube + (SPARE, dim), bf16),
                pltpu.VMEM((COLORS, SIDE, SIDE, SPARE, dim), bf16),
                pltpu.VMEM((COLORS, SIDE, SPARE, dim), bf16),
                pltpu.VMEM((COLORS, SIDE - 1, SIDE, SIDE, SPARE, dim), bf16),
                pltpu.VMEM((COLORS, SIDE - 1, SIDE, SPARE, dim), bf16),
                pltpu.VMEM((COLORS, SIDE - 1, SPARE, dim), bf16),
                pltpu.VMEM((128, dim), bf16),
                pltpu.VMEM((tok, 128), jnp.int32),
                pltpu.VMEM((tok, dim), jnp.float32),
                pairs, pairs, pairs, pairs, quads, quads, quads, quads, sems((3,)), sems((3,)),
            ],
            compiler_params=pltpu.CompilerParams(
                collective_id=0, has_side_effects=True, vmem_limit_bytes=67043328),
            name="layer",
        )(route, gate, x, w_gate, w_up, w_down)
        return lax.cond(flag[0, 0] > 0.0, wide, lambda *args: y, x, route, gate, w_gate, w_up, w_down)

    return jax.shard_map(
        device_step,
        mesh=mesh,
        in_specs=(tok_spec, tok_spec, tok_spec, expert_spec, expert_spec, expert_spec),
        out_specs=tok_spec,
        check_vma=False,
    )
```

```python
import functools

import jax
import jax.numpy as jnp
from jax import lax
from jax.experimental import pallas as pl
from jax.experimental.pallas import tpu as pltpu
from jax.sharding import PartitionSpec as P

MESH = pl.DeviceIdType.MESH
TILE = 256
VMEM_LIMIT = 60 * 1024 * 1024
COLORS = 3
PART = 4
BASE = COLORS * PART
SPARE = 8
OVER = COLORS * SPARE
SIDE = 4
TAIL = 128


def iota(shape, dim):
    return lax.broadcasted_iota(jnp.int32, shape, dim)


def ones_where(mask):
    return jnp.where(mask, 1.0, 0.0).astype(jnp.bfloat16)


def dot(a, b):
    return jnp.dot(a, b, preferred_element_type=jnp.float32)


def expert_ffn(rows, wg_ref, wu_ref, wd_ref):
    act_a = dot(rows, wg_ref[...])
    act_b = dot(rows, wu_ref[...])
    hidden = (jax.nn.silu(act_a) * act_b).astype(jnp.bfloat16)
    return dot(hidden, wd_ref[...]).astype(jnp.bfloat16)


def ranks(route0, route1, n_experts):
    tok = route0.shape[0]
    lanes = iota((tok, n_experts), 1)
    member0 = route0 == lanes
    member1 = route1 == lanes
    lower = ones_where(iota((tok, tok), 0) >= iota((tok, tok), 1))
    rank0 = dot(lower, ones_where(member0))
    rank1 = dot(lower, ones_where(member1)) + rank0[tok - 1:tok, :]
    return member0, member1, rank0 - 1.0, rank1 - 1.0, rank1[tok - 1:tok, :]


def as_row(column):
    return jnp.transpose(jnp.broadcast_to(column, (column.shape[0], 128)))[0:1, :]


def wide_pack_kernel(cap, route_ref, x_ref, send_ref, pos_ref):
    tok = x_ref.shape[0]
    rows = send_ref.shape[0]
    member0, member1, rank0, rank1, _ = ranks(route_ref[:, 0:1], route_ref[:, 1:2], rows // cap)
    base = (iota(member0.shape, 1) * cap).astype(jnp.float32)
    pos0 = jnp.sum(jnp.where(member0, rank0 + base, 0.0), axis=1, keepdims=True)
    pos1 = jnp.sum(jnp.where(member1, rank1 + base, 0.0), axis=1, keepdims=True)
    pos_ref[...] = jnp.concatenate([pos0, pos1], axis=1).astype(jnp.int32)
    row0, row1 = as_row(pos0), as_row(pos1)

    def block(i, carry):
        place = (iota((TILE, tok), 0) + i * TILE).astype(jnp.float32)
        pick = ones_where((place == row0) | (place == row1))
        send_ref[pl.ds(pl.multiple_of(i * TILE, TILE), TILE), :] = dot(pick, x_ref[...]).astype(jnp.bfloat16)
        return carry

    lax.fori_loop(0, rows // TILE, block, 0)


def wide_ffn_kernel(x_ref, wg_ref, wu_ref, wd_ref, o_ref):
    o_ref[...] = expert_ffn(x_ref[...], wg_ref, wu_ref, wd_ref)


def wide_mix_kernel(ret_ref, pos_ref, gate_ref, y_ref):
    n_rows = ret_ref.shape[0]

    def block(i, carry):
        part = pl.ds(pl.multiple_of(i * TILE, TILE), TILE)
        lanes = iota((TILE, n_rows), 1)
        total = gate_ref[part, 0:1] * dot(ones_where(pos_ref[part, 0:1] == lanes), ret_ref[...])
        total = total + gate_ref[part, 1:2] * dot(ones_where(pos_ref[part, 1:2] == lanes), ret_ref[...])
        y_ref[part, :] = total.astype(jnp.bfloat16)
        return carry

    lax.fori_loop(0, y_ref.shape[0] // TILE, block, 0)


class Torus:
    def __init__(self):
        self.sub = lax.axis_index("sub")
        ep = lax.axis_index("ep")
        self.at = (ep % SIDE, (ep // SIDE) % SIDE, ep // (SIDE * SIDE))

    def coord(self, axis, step):
        return (self.at[axis] + step) % SIDE

    def device(self, axis, step, core=0):
        at = list(self.at)
        at[axis] = self.coord(axis, step)
        return {"sub": (self.sub + core) % 2, "ep": (at[2] * SIDE + at[1]) * SIDE + at[0]}

    def greet(self):
        barrier = pltpu.get_barrier_semaphore()
        peers = [self.device(0, 0, 1)]
        for axis in range(3):
            for step in range(1, SIDE):
                for core in range(2):
                    peers.append(self.device(axis, step, core))
        for peer in peers:
            pl.semaphore_signal(barrier, inc=1, device_id=peer, device_id_type=MESH)
        return lambda: pl.semaphore_wait(barrier, len(peers))


def remote(src, dst, send_sem, recv_sem, device):
    return pltpu.make_async_remote_copy(
        src_ref=src, dst_ref=dst, send_sem=send_sem, recv_sem=recv_sem, device_id=device, device_id_type=MESH)


def start(copies):
    for copy in copies:
        copy.start()


def arrive(copies):
    for copy in copies:
        copy.wait_recv()


def settle(copies):
    for copy in copies:
        if copy.is_remote:
            copy.wait_send()


def at(i, table):
    for j, steps in table.items():
        @pl.when(i == j)
        def _(steps=steps):
            for step in steps:
                step()


STEPS = (1, 3, 2)
CHUNKS = [(k, h) for h in range(2) for k in range(COLORS)]


def layer_kernel(route_ref, gate_ref, x_ref, wg_hbm, wu_hbm, wd_hbm, y_ref, flag_ref,
                 wg, wu, wd, a, b, c, d, cc, bb, aa, every, late, stage, sum2, sum1, relay, got3, got2, got1, last,
                 cols, total, send, recv, bsend, brecv, esend, erecv, rsend, rrecv, wsem):
    tok, dim = x_ref.shape
    rows = 2 * SIDE ** 3 * PART
    t = Torus()
    s = t.sub
    load = [pltpu.make_async_copy(src, dst, wsem.at[i])
            for i, (src, dst) in enumerate(((wg_hbm, wg), (wu_hbm, wu), (wd_hbm, wd)))]
    start(load)
    everyone_here = t.greet()

    def place(k):
        return tuple(t.at[(k + i) % 3] for i in range(3))

    def out(phase, k, h):
        ax, sh = (k + phase) % 3, (s + h) % 2
        c1, c2, c3 = place(k)
        copies = []
        for step in STEPS + (0,):
            to = t.coord(ax, step)
            core = h if phase == 0 else 0
            if phase == 0:
                src, dst = a.at[k, sh, to], b.at[k, s, c1]
            elif phase == 1:
                src, dst = b.at[k, sh, :, to], c.at[k, sh, c2]
            else:
                src, dst = c.at[k, sh, :, :, to], d.at[k, sh, c3]
            if step == 0 and core == 0:
                copies.append(pltpu.make_async_copy(src, dst, recv.at[phase, k, h, step]))
            else:
                copies.append(remote(src, dst, send.at[phase, k, h, step], recv.at[phase, k, h, step],
                                     t.device(ax, step, core)))
        return copies

    def back(phase, k, h):
        ax, sh = (k + phase) % 3, (s + h) % 2
        c1, c2, c3 = place(k)
        copies = []
        for step in STEPS + (0,):
            to = t.coord(ax, step)
            core = h if phase == 0 else 0
            if phase == 0:
                src, dst = bb.at[k, sh, to], aa.at[k, s, c1]
            elif phase == 1:
                src, dst = cc.at[k, sh, to], bb.at[k, sh, :, c2]
            else:
                src, dst = d.at[k, sh, to], cc.at[k, sh, :, :, c3]
            if step == 0 and core == 0:
                copies.append(pltpu.make_async_copy(src, dst, brecv.at[phase, k, h, step]))
            else:
                copies.append(remote(src, dst, bsend.at[phase, k, h, step], brecv.at[phase, k, h, step],
                                     t.device(ax, step, core)))
        return copies

    def gather(phase, k):
        c1, c2, c3 = place(k)
        if phase == 3:
            part = every.at[s, k]
            return [remote(part, part, esend.at[3, k, 0], erecv.at[3, k, 0], t.device(0, 0, 1))]
        if phase == 4:
            copies = []
            for step, part in ((1, slice(0, SIDE // 2)), (3, slice(SIDE // 2, SIDE))):
                far = every.at[s, k, part, :, t.coord((k + 2) % 3, -step)]
                copies.append(remote(far, far, esend.at[4, k, step], erecv.at[4, k, step], t.device((k + 2) % 3, step)))
            return copies
        mine = (every.at[s, k, c1, c2, c3], every.at[s, k, :, c2, c3], every.at[s, k, :, :, c3])[phase]
        return [remote(mine, mine, esend.at[phase, k, step], erecv.at[phase, k, step],
                       t.device((k + phase) % 3, step)) for step in (STEPS[:2] if phase == 2 else STEPS)]

    def reduce(phase, k):
        if phase == 3:
            return [remote(late.at[1 - s, k], stage.at[k], rsend.at[3, k, 0], rrecv.at[3, k, 0], t.device(0, 0, 1))]
        copies = []
        if phase == 4:
            far = t.coord((k + 2) % 3, 2)
            for i, (step, part) in enumerate(((1, slice(0, SIDE // 2)), (3, slice(SIDE // 2, SIDE)))):
                copies.append(remote(late.at[s, k, part, :, far], relay.at[k, i], rsend.at[4, k, step],
                                     rrecv.at[4, k, step], t.device((k + 2) % 3, step)))
            return copies
        for step in STEPS[:2] if phase == 2 else STEPS:
            to = t.coord((k + phase) % 3, step)
            src = (sum1.at[k, to], sum2.at[k, :, to], late.at[s, k, :, :, to])[phase]
            dst = (got1, got2, got3)[phase].at[k, step // 2 if phase == 2 else step - 1]
            copies.append(remote(src, dst, rsend.at[phase, k, step], rrecv.at[phase, k, step],
                                 t.device((k + phase) % 3, step)))
        return copies

    def merge(phase, k):
        if phase == 3:
            def add(i, carry):
                late[s, k, i] = late[s, k, i] + stage[k, i]
                return carry

            lax.fori_loop(0, SIDE, add, 0)
            return
        if phase == 4:
            right, left = t.coord((k + 2) % 3, 1), t.coord((k + 2) % 3, 3)
            late[s, k, 0:SIDE // 2, :, right] = late[s, k, 0:SIDE // 2, :, right] + relay[k, 0]
            late[s, k, SIDE // 2:SIDE, :, left] = late[s, k, SIDE // 2:SIDE, :, left] + relay[k, 1]
            return
        mine = t.at[(k + phase) % 3]
        got = (got1, got2, got3)[phase]
        more = got[k, 0] + got[k, 1]
        if phase < 2:
            more = more + got[k, 2]
        if phase == 2:
            sum2[k] = late[s, k, :, :, mine] + more
        elif phase == 1:
            sum1[k] = sum2[k, :, mine] + more
        else:
            last[k * SPARE:(k + 1) * SPARE, :] = sum1[k, mine] + more

    n_experts = 2 * SIDE ** 3
    table = jnp.concatenate([route_ref[...].astype(jnp.float32), gate_ref[...], jnp.zeros((4, tok), jnp.float32)], axis=0)
    table = jnp.transpose(table)
    route0, route1 = table[:, 0:1].astype(jnp.int32), table[:, 1:2].astype(jnp.int32)
    gates = slice(2, 4)
    cols[:, gates] = table[:, gates]
    member0, member1, rank0, rank1, count = ranks(route0, route1, n_experts)
    lanes = iota((1, n_experts), 1)
    sub, ep = lanes // (SIDE ** 3), lanes % (SIDE ** 3)
    axes = (ep % SIDE, (ep // SIDE) % SIDE, ep // (SIDE * SIDE))
    first = []
    for k in range(COLORS):
        d1, d2, d3 = (axes[(k + i) % 3] for i in range(3))
        block = ((sub * SIDE + d1) * SIDE + d2) * SIDE + d3
        first.append((k * rows + block * PART - k * PART).astype(jnp.float32))
    excess = jnp.maximum(count - BASE, 0.0)
    strict = ones_where(iota((n_experts, n_experts), 0) < iota((n_experts, n_experts), 1))
    ahead = dot(jnp.broadcast_to(excess, (8, n_experts)).astype(jnp.bfloat16), strict)[0:1, :]
    n_over = jnp.sum(excess, axis=1, keepdims=True)
    nowhere = 4.0 * COLORS * rows

    def places(member, rank):
        base = jnp.where(rank < PART, first[0], jnp.where(rank < 2 * PART, first[1], first[2]))
        behind = ahead + (rank - BASE)
        where = jnp.where(rank < BASE, base + rank, jnp.where(behind < OVER, COLORS * rows + behind, nowhere))
        return jnp.sum(jnp.where(member, where, 0.0), axis=1, keepdims=True)

    pos0, pos1 = places(member0, rank0), places(member1, rank1)
    cols[:, 0:1] = pos0
    cols[:, 1:2] = pos1
    both = jnp.transpose(jnp.where(iota((tok, 128), 1) == 0, pos0, pos1))
    row0, row1 = both[0:1, :], both[1:2, :]

    def pack(i, carry):
        k, sh = i % COLORS, (s + i // COLORS) % 2
        spot = (iota((TILE, tok), 0) + (k * rows + sh * TILE)).astype(jnp.float32)
        pick = ones_where((spot == row0) | (spot == row1))
        got = dot(pick, x_ref[...]).astype(jnp.bfloat16)
        a[k, sh] = got.reshape(SIDE, SIDE, SIDE, PART, dim)
        events = {j + 1: [lambda q=q: start(out(0, *q))] for j, q in enumerate(CHUNKS[:-1])}
        events[1].insert(0, everyone_here)
        at(i, events)
        return carry

    lax.fori_loop(0, len(CHUNKS), pack, 0)

    spot = (iota((32, tok), 0) + COLORS * rows).astype(jnp.float32)
    pick0, pick1 = ones_where(spot == row0), ones_where(spot == row1)
    got = dot(pick0 + pick1, x_ref[...]).astype(jnp.bfloat16)
    expert0 = jnp.broadcast_to(route0 + 1, (tok, TAIL)).astype(jnp.bfloat16)
    expert1 = jnp.broadcast_to(route1 + 1, (tok, TAIL)).astype(jnp.bfloat16)
    owner = dot(pick0, expert0) + dot(pick1, expert1)
    flag = jnp.where(n_over > OVER, 1.0, 0.0)
    tail = jnp.where(iota((32, TAIL), 1) == 0, owner, flag).astype(jnp.bfloat16)
    for k in range(COLORS):
        c1, c2, c3 = place(k)
        part = slice(k * SPARE, (k + 1) * SPARE)
        every[s, k, c1, c2, c3, :, 0:dim] = got[part, :]
        every[s, k, c1, c2, c3, :, dim:dim + TAIL] = tail[part, :]
    start(out(0, *CHUNKS[-1]))
    for k in range(COLORS):
        start(gather(0, k))
    for phase in range(1, 3):
        for k, h in CHUNKS:
            arrive(out(phase - 1, k, h))
            start(out(phase, k, h))
        for k in range(COLORS):
            arrive(gather(phase - 1, k))
            start(gather(phase, k))
    arrive(load)

    def ffn(i, carry):
        k, h = i % COLORS, i // COLORS
        sh = (s + h) % 2
        at(i, {j: [lambda q=q: arrive(out(2, *q))] for j, q in enumerate(CHUNKS)})
        d[k, sh] = expert_ffn(d[k, sh].reshape(TILE, dim), wg, wu, wd).reshape(SIDE, SIDE, SIDE, PART, dim)
        at(i, {j: [lambda q=q: start(back(2, *q))] for j, q in enumerate(CHUNKS)})
        at(i, {j + 3: [lambda j=j: arrive(gather(2, j)), lambda j=j: start(gather(4, j))] for j in range(COLORS)})
        return carry

    lax.fori_loop(0, len(CHUNKS), ffn, 0)

    me = (s * SIDE ** 3 + lax.axis_index("ep") + 1).astype(jnp.float32)
    flag_ref[...] = jnp.zeros_like(flag_ref)
    order = [2, 4, 5, 7, 9, 10]

    def over_ffn(i, carry):
        core, k, part = (s + i // 6) % 2, (i // 2) % COLORS, (i % 2) * 2
        before = {2 * j: [lambda j=j: arrive(gather(4, j)), lambda j=j: start(gather(3, j))] for j in range(COLORS)}
        before.update({6 + 2 * j: [lambda j=j: arrive(gather(3, j))] for j in range(COLORS)})
        at(i, before)
        got = every[core, k, pl.ds(part, 2)].reshape(TILE, dim + TAIL)
        tail = got[:, dim:dim + TAIL].astype(jnp.float32)
        flag_ref[...] = jnp.maximum(flag_ref[...], jnp.max(tail[:, 1:2], axis=0, keepdims=True))
        result = expert_ffn(got[:, 0:dim], wg, wu, wd).astype(jnp.float32)
        result = jnp.where(tail[:, 0:1] == me, result, 0.0).astype(jnp.bfloat16)
        late[core, k, pl.ds(part, 2)] = result.reshape(2, SIDE, SIDE, SPARE, dim)
        at(i, {order[j]: [lambda q=q: arrive(back(2, *q)), lambda q=q: start(back(1, *q))]
               for j, q in enumerate(CHUNKS)})
        at(i, {8: [lambda: start(reduce(3, 0))]})
        return carry

    lax.fori_loop(0, 12, over_ffn, 0)
    start(reduce(3, 1))
    start(reduce(3, 2))
    for k in range(COLORS):
        arrive(reduce(3, k))
        merge(3, k)
        if k:
            start(reduce(4, k - 1))
    start(reduce(4, 2))
    for k, h in CHUNKS[:COLORS]:
        arrive(back(1, k, h))
        start(back(0, k, h))
    for k in range(COLORS):
        arrive(reduce(4, k))
        merge(4, k)
        if k:
            start(reduce(2, k - 1))
    start(reduce(2, 2))
    for k, h in CHUNKS[COLORS:]:
        arrive(back(1, k, h))
        start(back(0, k, h))
    for phase in (2, 1):
        for k in range(COLORS):
            arrive(reduce(phase, k))
            merge(phase, k)
            if k:
                start(reduce(phase - 1, k - 1))
        start(reduce(phase - 1, 2))
    total[...] = jnp.zeros_like(total)

    def mix(i, carry):
        k, sh = i % COLORS, (s + i // COLORS) % 2
        at(i, {j: [lambda q=q: arrive(back(0, *q))] for j, q in enumerate(CHUNKS)})
        got = aa[k, sh].reshape(TILE, dim)
        lanes = (iota((TILE, TILE), 1) + (k * rows + sh * TILE)).astype(jnp.float32)
        for part in range(tok // TILE):
            where = pl.ds(part * TILE, TILE)
            add = cols[where, 2:3] * dot(ones_where(cols[where, 0:1] == lanes), got)
            total[where, :] += add + cols[where, 3:4] * dot(ones_where(cols[where, 1:2] == lanes), got)
        return carry

    lax.fori_loop(0, len(CHUNKS), mix, 0)
    last[...] = jnp.zeros_like(last)
    for k in range(COLORS):
        arrive(reduce(0, k))
        merge(0, k)
    lanes = (iota((TILE, last.shape[0]), 1) + COLORS * rows).astype(jnp.float32)
    for part in range(tok // TILE):
        where = pl.ds(part * TILE, TILE)
        add = cols[where, 2:3] * dot(ones_where(cols[where, 0:1] == lanes), last[...])
        add = add + cols[where, 3:4] * dot(ones_where(cols[where, 1:2] == lanes), last[...])
        y_ref[where, :] = (total[where, :] + add).astype(jnp.bfloat16)
    for k in range(COLORS):
        for phase in range(3):
            for h in range(2):
                settle(out(phase, k, h) + back(phase, k, h))
        for phase in range(5):
            settle(gather(phase, k) + reduce(phase, k))


def solution(mesh):
    n_sub, n_ep = mesh.shape["sub"], mesh.shape["ep"]
    n_dev = n_sub * n_ep
    tok_spec = P(("dp", "sub", "ep"), None)
    expert_spec = P(("sub", "ep"), None, None)
    group = ("sub", "ep")
    vmem = pl.BlockSpec(memory_space=pltpu.VMEM)
    hbm = pl.BlockSpec(memory_space=pl.ANY)
    params = pltpu.CompilerParams(vmem_limit_bytes=VMEM_LIMIT)
    bf16 = jnp.bfloat16

    def shape(*dims):
        return jax.ShapeDtypeStruct(dims, bf16)

    def weights(dim, ff):
        return [
            pl.BlockSpec((dim, ff), lambda i: (0, 0)),
            pl.BlockSpec((dim, ff), lambda i: (0, 0)),
            pl.BlockSpec((ff, dim), lambda i: (0, 0)),
        ]

    def wide(x, route, gate, w_gate, w_up, w_down):
        tok, dim = x.shape
        ff = w_gate.shape[1]
        cap = min(tok, 8 * tok // n_dev)
        rows = n_dev * cap
        send, pos = pl.pallas_call(
            functools.partial(wide_pack_kernel, cap),
            out_shape=[shape(rows, dim), jax.ShapeDtypeStruct((tok, 2), jnp.int32)],
            in_specs=[vmem, vmem],
            out_specs=[vmem, vmem],
            compiler_params=params,
            name="wide_pack",
        )(route, x)
        got = lax.all_to_all(send.reshape(n_dev, cap, dim), group, 0, 0).reshape(rows, dim)
        block = pl.BlockSpec((TILE, dim), lambda i: (i, 0))
        out = pl.pallas_call(
            wide_ffn_kernel,
            out_shape=shape(rows, dim),
            grid=(rows // TILE,),
            in_specs=[block] + weights(dim, ff),
            out_specs=block,
            compiler_params=params,
            name="wide_ffn",
        )(got, w_gate, w_up, w_down)
        ret = lax.all_to_all(out.reshape(n_dev, cap, dim), group, 0, 0).reshape(rows, dim)
        return pl.pallas_call(
            wide_mix_kernel,
            out_shape=shape(tok, dim),
            in_specs=[vmem, vmem, vmem],
            out_specs=vmem,
            compiler_params=params,
            name="wide_mix",
        )(ret, pos, gate)

    cube = (SIDE, SIDE, SIDE)

    def device_step(x, route, gate, w_gate, w_up, w_down):
        tok, dim = x.shape
        ff = w_gate.shape[2]
        w_gate, w_up, w_down = w_gate[0], w_up[0], w_down[0]
        sems = pltpu.SemaphoreType.DMA
        main = pltpu.VMEM((COLORS, 2) + cube + (PART, dim), bf16)
        pairs = sems((3, COLORS, 2, SIDE))
        quads = sems((5, COLORS, SIDE))
        y, flag = pl.pallas_call(
            layer_kernel,
            out_shape=[shape(tok, dim), jax.ShapeDtypeStruct((1, 1), jnp.float32)],
            in_specs=[vmem, vmem, vmem, hbm, hbm, hbm],
            out_specs=[vmem, vmem],
            scratch_shapes=[
                pltpu.VMEM((dim, ff), bf16), pltpu.VMEM((dim, ff), bf16), pltpu.VMEM((ff, dim), bf16),
                main, main, main, main, main, main, main,
                pltpu.VMEM((2, COLORS) + cube + (SPARE, dim + TAIL), bf16),
                pltpu.VMEM((2, COLORS) + cube + (SPARE, dim), bf16),
                pltpu.VMEM((COLORS,) + cube + (SPARE, dim), bf16),
                pltpu.VMEM((COLORS, SIDE, SIDE, SPARE, dim), bf16),
                pltpu.VMEM((COLORS, SIDE, SPARE, dim), bf16),
                pltpu.VMEM((COLORS, 2, SIDE // 2, SIDE, SPARE, dim), bf16),
                pltpu.VMEM((COLORS, 2, SIDE, SIDE, SPARE, dim), bf16),
                pltpu.VMEM((COLORS, SIDE - 1, SIDE, SPARE, dim), bf16),
                pltpu.VMEM((COLORS, SIDE - 1, SPARE, dim), bf16),
                pltpu.VMEM((128, dim), bf16),
                pltpu.VMEM((tok, 128), jnp.float32),
                pltpu.VMEM((tok, dim), jnp.float32),
                pairs, pairs, pairs, pairs, quads, quads, quads, quads, sems((3,)),
            ],
            compiler_params=pltpu.CompilerParams(
                collective_id=0, has_side_effects=True, vmem_limit_bytes=67043328),
            name="layer",
        )(route.T, gate.T, x, w_gate, w_up, w_down)
        return lax.cond(flag[0, 0] > 0.0, wide, lambda *args: y, x, route, gate, w_gate, w_up, w_down)

    return jax.shard_map(
        device_step,
        mesh=mesh,
        in_specs=(tok_spec, tok_spec, tok_spec, expert_spec, expert_spec, expert_spec),
        out_specs=tok_spec,
        check_vma=False,
    )
```

```python
import functools

import jax
import jax.numpy as jnp
from jax import lax
from jax.experimental import pallas as pl
from jax.experimental.pallas import tpu as pltpu
from jax.sharding import PartitionSpec as P

MESH = pl.DeviceIdType.MESH
TILE = 256
VMEM_LIMIT = 60 * 1024 * 1024
COLORS = 3
PART = 4
BASE = COLORS * PART
SPARE = 8
OVER = COLORS * SPARE
SIDE = 4
TAIL = 128


def iota(shape, dim):
    return lax.broadcasted_iota(jnp.int32, shape, dim)


def ones_where(mask):
    return jnp.where(mask, 1.0, 0.0).astype(jnp.bfloat16)


def dot(a, b):
    return jnp.dot(a, b, preferred_element_type=jnp.float32)


def expert_ffn(rows, wg_ref, wu_ref, wd_ref):
    act_a = dot(rows, wg_ref[...])
    act_b = dot(rows, wu_ref[...])
    hidden = (jax.nn.silu(act_a) * act_b).astype(jnp.bfloat16)
    return dot(hidden, wd_ref[...]).astype(jnp.bfloat16)


def ranks(route0, route1, n_experts):
    tok = route0.shape[0]
    lanes = iota((tok, n_experts), 1)
    member0 = route0 == lanes
    member1 = route1 == lanes
    lower = ones_where(iota((tok, tok), 0) >= iota((tok, tok), 1))
    rank0 = dot(lower, ones_where(member0))
    rank1 = dot(lower, ones_where(member1)) + rank0[tok - 1:tok, :]
    return member0, member1, rank0 - 1.0, rank1 - 1.0, rank1[tok - 1:tok, :]


def as_row(column):
    return jnp.transpose(jnp.broadcast_to(column, (column.shape[0], 128)))[0:1, :]


def wide_pack_kernel(cap, route_ref, x_ref, send_ref, pos_ref):
    tok = x_ref.shape[0]
    rows = send_ref.shape[0]
    member0, member1, rank0, rank1, _ = ranks(route_ref[:, 0:1], route_ref[:, 1:2], rows // cap)
    base = (iota(member0.shape, 1) * cap).astype(jnp.float32)
    pos0 = jnp.sum(jnp.where(member0, rank0 + base, 0.0), axis=1, keepdims=True)
    pos1 = jnp.sum(jnp.where(member1, rank1 + base, 0.0), axis=1, keepdims=True)
    pos_ref[...] = jnp.concatenate([pos0, pos1], axis=1).astype(jnp.int32)
    row0, row1 = as_row(pos0), as_row(pos1)

    def block(i, carry):
        place = (iota((TILE, tok), 0) + i * TILE).astype(jnp.float32)
        pick = ones_where((place == row0) | (place == row1))
        send_ref[pl.ds(pl.multiple_of(i * TILE, TILE), TILE), :] = dot(pick, x_ref[...]).astype(jnp.bfloat16)
        return carry

    lax.fori_loop(0, rows // TILE, block, 0)


def wide_ffn_kernel(x_ref, wg_ref, wu_ref, wd_ref, o_ref):
    o_ref[...] = expert_ffn(x_ref[...], wg_ref, wu_ref, wd_ref)


def wide_mix_kernel(ret_ref, pos_ref, gate_ref, y_ref):
    n_rows = ret_ref.shape[0]

    def block(i, carry):
        part = pl.ds(pl.multiple_of(i * TILE, TILE), TILE)
        lanes = iota((TILE, n_rows), 1)
        total = gate_ref[part, 0:1] * dot(ones_where(pos_ref[part, 0:1] == lanes), ret_ref[...])
        total = total + gate_ref[part, 1:2] * dot(ones_where(pos_ref[part, 1:2] == lanes), ret_ref[...])
        y_ref[part, :] = total.astype(jnp.bfloat16)
        return carry

    lax.fori_loop(0, y_ref.shape[0] // TILE, block, 0)


class Torus:
    def __init__(self):
        self.sub = lax.axis_index("sub")
        ep = lax.axis_index("ep")
        self.at = (ep % SIDE, (ep // SIDE) % SIDE, ep // (SIDE * SIDE))

    def coord(self, axis, step):
        return (self.at[axis] + step) % SIDE

    def device(self, axis, step, core=0):
        at = list(self.at)
        at[axis] = self.coord(axis, step)
        return {"sub": (self.sub + core) % 2, "ep": (at[2] * SIDE + at[1]) * SIDE + at[0]}

    def greet(self):
        barrier = pltpu.get_barrier_semaphore()
        peers = [self.device(0, 0, 1)]
        for axis in range(3):
            for step in range(1, SIDE):
                for core in range(2):
                    peers.append(self.device(axis, step, core))
        for peer in peers:
            pl.semaphore_signal(barrier, inc=1, device_id=peer, device_id_type=MESH)
        return lambda: pl.semaphore_wait(barrier, len(peers))


def remote(src, dst, send_sem, recv_sem, device):
    return pltpu.make_async_remote_copy(
        src_ref=src, dst_ref=dst, send_sem=send_sem, recv_sem=recv_sem, device_id=device, device_id_type=MESH)


def start(copies):
    for copy in copies:
        copy.start()


def drain(ref, sem):
    pltpu.make_async_copy(ref, ref, sem).wait()


def at(i, table):
    for j, steps in table.items():
        @pl.when(i == j)
        def _(steps=steps):
            for step in steps:
                step()


STEPS = (1, 3, 2)
CHUNKS = [(k, h) for h in range(2) for k in range(COLORS)]


def layer_kernel(route_ref, gate_ref, x_ref, wg_hbm, wu_hbm, wd_hbm, y_ref, flag_ref,
                 wg, wu, wd, a, b, c, d, cc, bb, aa, every, late, stage, sum2, sum1, relay, got3, got2, got1, last,
                 cols, total, send, recv, bsend, brecv, esend, erecv, rsend, rrecv, wsem):
    tok, dim = x_ref.shape
    rows = 2 * SIDE ** 3 * PART
    t = Torus()
    s = t.sub
    weights = [(src, dst, wsem.at[i]) for i, (src, dst) in enumerate(((wg_hbm, wg), (wu_hbm, wu), (wd_hbm, wd)))]
    for src, dst, sem in weights:
        pltpu.make_async_copy(src, dst, sem).start()
    everyone_here = t.greet()

    def place(k):
        return tuple(t.at[(k + i) % 3] for i in range(3))

    def out(phase, k, h):
        ax, sh = (k + phase) % 3, (s + h) % 2
        c1, c2, c3 = place(k)
        copies = []
        for step in STEPS + (0,):
            to = t.coord(ax, step)
            core = h if phase == 0 else 0
            if phase == 0:
                src, dst = a.at[k, sh, to], b.at[k, s, c1]
            elif phase == 1:
                src, dst = b.at[k, sh, :, to], c.at[k, sh, c2]
            else:
                src, dst = c.at[k, sh, :, :, to], d.at[k, sh, c3]
            if step == 0 and core == 0:
                copies.append(pltpu.make_async_copy(src, dst, recv.at[phase, k, h]))
            else:
                copies.append(remote(src, dst, send.at[phase, h], recv.at[phase, k, h], t.device(ax, step, core)))
        return copies

    def back(phase, k, h):
        ax, sh = (k + phase) % 3, (s + h) % 2
        c1, c2, c3 = place(k)
        copies = []
        for step in STEPS + (0,):
            to = t.coord(ax, step)
            core = h if phase == 0 else 0
            if phase == 0:
                src, dst = bb.at[k, sh, to], aa.at[k, s, c1]
            elif phase == 1:
                src, dst = cc.at[k, sh, to], bb.at[k, sh, :, c2]
            else:
                src, dst = d.at[k, sh, to], cc.at[k, sh, :, :, c3]
            if step == 0 and core == 0:
                copies.append(pltpu.make_async_copy(src, dst, brecv.at[phase, k, h]))
            else:
                copies.append(remote(src, dst, bsend.at[phase, h], brecv.at[phase, k, h], t.device(ax, step, core)))
        return copies

    def gather(phase, k):
        c1, c2, c3 = place(k)
        if phase == 3:
            part = every.at[s, k]
            return [remote(part, part, esend.at[3], erecv.at[3, k], t.device(0, 0, 1))]
        if phase == 4:
            copies = []
            for step, part in ((1, slice(0, SIDE // 2)), (3, slice(SIDE // 2, SIDE))):
                far = every.at[s, k, part, :, t.coord((k + 2) % 3, -step)]
                copies.append(remote(far, far, esend.at[4], erecv.at[4, k], t.device((k + 2) % 3, step)))
            return copies
        mine = (every.at[s, k, c1, c2, c3], every.at[s, k, :, c2, c3], every.at[s, k, :, :, c3])[phase]
        return [remote(mine, mine, esend.at[phase], erecv.at[phase, k], t.device((k + phase) % 3, step))
                for step in (STEPS[:2] if phase == 2 else STEPS)]

    def gathered(k):
        return (every.at[0, k, 0:3, 0, 0], every.at[0, k, 0:3, :, 0], every.at[0, k, 0:2], every.at[0, k],
                every.at[0, k, 0:1])

    def reduce(phase, k):
        if phase == 3:
            return [remote(late.at[1 - s, k], stage.at[k], rsend.at[3], rrecv.at[3, k], t.device(0, 0, 1))]
        copies = []
        if phase == 4:
            far = t.coord((k + 2) % 3, 2)
            for i, (step, part) in enumerate(((1, slice(0, SIDE // 2)), (3, slice(SIDE // 2, SIDE)))):
                copies.append(remote(late.at[s, k, part, :, far], relay.at[k, i], rsend.at[4],
                                     rrecv.at[4, k], t.device((k + 2) % 3, step)))
            return copies
        for step in STEPS[:2] if phase == 2 else STEPS:
            to = t.coord((k + phase) % 3, step)
            src = (sum1.at[k, to], sum2.at[k, :, to], late.at[s, k, :, :, to])[phase]
            dst = (got1, got2, got3)[phase].at[k, step // 2 if phase == 2 else step - 1]
            copies.append(remote(src, dst, rsend.at[phase], rrecv.at[phase, k], t.device((k + phase) % 3, step)))
        return copies

    def merge(phase, k):
        if phase == 3:
            def add(i, carry):
                late[s, k, i] = late[s, k, i] + stage[k, i]
                return carry

            lax.fori_loop(0, SIDE, add, 0)
            return
        if phase == 4:
            right, left = t.coord((k + 2) % 3, 1), t.coord((k + 2) % 3, 3)
            late[s, k, 0:SIDE // 2, :, right] = late[s, k, 0:SIDE // 2, :, right] + relay[k, 0]
            late[s, k, SIDE // 2:SIDE, :, left] = late[s, k, SIDE // 2:SIDE, :, left] + relay[k, 1]
            return
        mine = t.at[(k + phase) % 3]
        got = (got1, got2, got3)[phase]
        more = got[k, 0] + got[k, 1]
        if phase < 2:
            more = more + got[k, 2]
        if phase == 2:
            sum2[k] = late[s, k, :, :, mine] + more
        elif phase == 1:
            sum1[k] = sum2[k, :, mine] + more
        else:
            last[k * SPARE:(k + 1) * SPARE, :] = sum1[k, mine] + more

    n_experts = 2 * SIDE ** 3
    table = jnp.concatenate([route_ref[...].astype(jnp.float32), gate_ref[...], jnp.zeros((4, tok), jnp.float32)], axis=0)
    table = jnp.transpose(table)
    route0, route1 = table[:, 0:1].astype(jnp.int32), table[:, 1:2].astype(jnp.int32)
    gates = slice(2, 4)
    cols[:, gates] = table[:, gates]
    member0, member1, rank0, rank1, count = ranks(route0, route1, n_experts)
    lanes = iota((1, n_experts), 1)
    sub, ep = lanes // (SIDE ** 3), lanes % (SIDE ** 3)
    axes = (ep % SIDE, (ep // SIDE) % SIDE, ep // (SIDE * SIDE))
    first = []
    for k in range(COLORS):
        d1, d2, d3 = (axes[(k + i) % 3] for i in range(3))
        block = ((sub * SIDE + d1) * SIDE + d2) * SIDE + d3
        first.append((k * rows + block * PART - k * PART).astype(jnp.float32))
    excess = jnp.maximum(count - BASE, 0.0)
    strict = ones_where(iota((n_experts, n_experts), 0) < iota((n_experts, n_experts), 1))
    ahead = dot(jnp.broadcast_to(excess, (8, n_experts)).astype(jnp.bfloat16), strict)[0:1, :]
    n_over = jnp.sum(excess, axis=1, keepdims=True)
    nowhere = 4.0 * COLORS * rows

    def places(member, rank):
        base = jnp.where(rank < PART, first[0], jnp.where(rank < 2 * PART, first[1], first[2]))
        behind = ahead + (rank - BASE)
        where = jnp.where(rank < BASE, base + rank, jnp.where(behind < OVER, COLORS * rows + behind, nowhere))
        return jnp.sum(jnp.where(member, where, 0.0), axis=1, keepdims=True)

    pos0, pos1 = places(member0, rank0), places(member1, rank1)
    cols[:, 0:1] = pos0
    cols[:, 1:2] = pos1
    both = jnp.transpose(jnp.where(iota((tok, 128), 1) == 0, pos0, pos1))
    row0, row1 = both[0:1, :], both[1:2, :]

    spot = (iota((32, tok), 0) + COLORS * rows).astype(jnp.float32)
    pick0, pick1 = ones_where(spot == row0), ones_where(spot == row1)
    got = dot(pick0 + pick1, x_ref[...]).astype(jnp.bfloat16)
    expert0 = jnp.broadcast_to(route0 + 1, (tok, TAIL)).astype(jnp.bfloat16)
    expert1 = jnp.broadcast_to(route1 + 1, (tok, TAIL)).astype(jnp.bfloat16)
    owner = dot(pick0, expert0) + dot(pick1, expert1)
    flag = jnp.where(n_over > OVER, 1.0, 0.0)
    tail = jnp.where(iota((32, TAIL), 1) == 0, owner, flag).astype(jnp.bfloat16)
    for k in range(COLORS):
        c1, c2, c3 = place(k)
        part = slice(k * SPARE, (k + 1) * SPARE)
        every[s, k, c1, c2, c3, :, 0:dim] = got[part, :]
        every[s, k, c1, c2, c3, :, dim:dim + TAIL] = tail[part, :]
    def relay_gather(phase, k):
        drain(gathered(k)[phase], erecv.at[phase, k])
        start(gather({0: 1, 1: 2, 2: 4, 4: 3}[phase], k))

    def relay_out(phase, k, h):
        drain(d.at[k, 0], recv.at[phase, k, h])
        start(out(phase + 1, k, h))

    def relay_back(phase, k, h):
        drain(d.at[k, 0], brecv.at[phase, k, h])
        start(back(phase - 1, k, h))

    def relay_reduce(phase, k):
        drain((got1, got2, got3, stage, relay)[phase].at[k], rrecv.at[phase, k])
        merge(phase, k)
        if phase:
            start(reduce({3: 4, 4: 2, 2: 1, 1: 0}[phase], k))

    firsts, seconds = CHUNKS[:COLORS], CHUNKS[COLORS:]

    def pack(i, carry):
        k, sh = i % COLORS, (s + i // COLORS) % 2
        spot = (iota((TILE, tok), 0) + (k * rows + sh * TILE)).astype(jnp.float32)
        pick = ones_where((spot == row0) | (spot == row1))
        got = dot(pick, x_ref[...]).astype(jnp.bfloat16)
        a[k, sh] = got.reshape(SIDE, SIDE, SIDE, PART, dim)
        events = {j + 1: [lambda q=q: start(out(0, *q))] for j, q in enumerate(firsts)}
        events[1] = [everyone_here] + [lambda k=k: start(gather(0, k)) for k in range(COLORS)] + events[1]
        at(i, events)
        return carry

    lax.fori_loop(0, len(CHUNKS), pack, 0)
    for k in range(COLORS):
        relay_gather(0, k)
    for q in seconds:
        start(out(0, *q))
    for k in range(COLORS):
        relay_gather(1, k)
    for q in firsts:
        relay_out(0, *q)
    for k in range(COLORS):
        relay_gather(2, k)
    for q in seconds:
        relay_out(0, *q)
    for q in firsts:
        relay_out(1, *q)
    for src, dst, sem in weights:
        pltpu.make_async_copy(src, dst, sem).wait()
    me = (s * SIDE ** 3 + lax.axis_index("ep") + 1).astype(jnp.float32)
    flag_ref[...] = jnp.zeros_like(flag_ref)

    over_steps, main_steps = (0, 1, 2, 3, 4, 8), (5, 6, 7, 9, 10, 11)
    before = {j: [lambda q=q: drain(d.at[q[0], 0], recv.at[2, q[0], q[1]])] for j, q in zip(main_steps, CHUNKS)}
    before.update({over_steps[COLORS + k]: [lambda k=k: drain(gathered(k)[3], erecv.at[3, k])] for k in range(COLORS)})
    before[0] = [lambda k=k: relay_gather(4, k) for k in range(COLORS)]
    before[4].insert(0, lambda: start(reduce(3, 0)))
    before[5].insert(0, lambda: start(reduce(3, 1)))
    before[9].insert(0, lambda: start(reduce(3, 2)))
    after = {j: [lambda q=q: start(back(2, *q))] for j, q in zip(main_steps, CHUNKS)}
    after[2] = [lambda q=q: relay_out(1, *q) for q in seconds]
    after[6].append(lambda: relay_reduce(3, 0))
    after[9].append(lambda: relay_reduce(3, 1))
    after[11].append(lambda: relay_reduce(3, 2))

    def work(i, carry):
        at(i, before)
        is_over = (i < 5) | (i == 8)

        @pl.when(is_over)
        def _():
            j = jnp.where(i == 8, 5, i)
            core, k = (s + j // COLORS) % 2, j % COLORS
            got = every[core, k].reshape(2 * TILE, dim + TAIL)
            tail = got[:, dim:dim + TAIL].astype(jnp.float32)
            flag_ref[...] = jnp.maximum(flag_ref[...], jnp.max(tail[:, 1:2], axis=0, keepdims=True))
            result = expert_ffn(got[:, 0:dim], wg, wu, wd).astype(jnp.float32)
            result = jnp.where(tail[:, 0:1] == me, result, 0.0).astype(jnp.bfloat16)
            late[core, k] = result.reshape(SIDE, SIDE, SIDE, SPARE, dim)

        @pl.when(jnp.logical_not(is_over))
        def _():
            j = jnp.where(i < 8, i - 5, i - 6)
            k, sh = j % COLORS, (s + j // COLORS) % 2
            d[k, sh] = expert_ffn(d[k, sh].reshape(TILE, dim), wg, wu, wd).reshape(SIDE, SIDE, SIDE, PART, dim)

        at(i, after)
        return carry

    lax.fori_loop(0, 12, work, 0)
    for q in firsts:
        relay_back(2, *q)
    for k in range(COLORS):
        relay_reduce(4, k)
    for q in seconds:
        relay_back(2, *q)
    for k in range(COLORS):
        relay_reduce(2, k)
    for q in firsts:
        relay_back(1, *q)
    for k in range(COLORS):
        relay_reduce(1, k)
    for q in seconds:
        relay_back(1, *q)
    last[...] = jnp.zeros_like(last)
    for k in range(COLORS):
        relay_reduce(0, k)
    lanes = (iota((TILE, last.shape[0]), 1) + COLORS * rows).astype(jnp.float32)
    for part in range(tok // TILE):
        where = pl.ds(part * TILE, TILE)
        add = cols[where, 2:3] * dot(ones_where(cols[where, 0:1] == lanes), last[...])
        total[where, :] = add + cols[where, 3:4] * dot(ones_where(cols[where, 1:2] == lanes), last[...])

    def mix(i, carry):
        k, sh = i % COLORS, (s + i // COLORS) % 2
        at(i, {j: [lambda q=q: drain(d.at[q[0], 0], brecv.at[0, q[0], q[1]])] for j, q in enumerate(CHUNKS)})
        got = aa[k, sh].reshape(TILE, dim)
        lanes = (iota((TILE, TILE), 1) + (k * rows + sh * TILE)).astype(jnp.float32)
        for part in range(tok // TILE):
            where = pl.ds(part * TILE, TILE)
            add = cols[where, 2:3] * dot(ones_where(cols[where, 0:1] == lanes), got)
            total[where, :] += add + cols[where, 3:4] * dot(ones_where(cols[where, 1:2] == lanes), got)
        return carry

    lax.fori_loop(0, len(CHUNKS), mix, 0)
    y_ref[...] = total[...].astype(jnp.bfloat16)
    for phase in range(3):
        for h in range(2):
            sent = d.at[:, 0] if phase == 0 and h else d.at[:, 0, 0:3]
            drain(sent, send.at[phase, h])
            drain(sent, bsend.at[phase, h])
    for phase in range(5):
        drain(gathered(slice(None))[phase], esend.at[phase])
        drain((got1, got2, got3, stage, relay)[phase], rsend.at[phase])


def solution(mesh):
    n_sub, n_ep = mesh.shape["sub"], mesh.shape["ep"]
    n_dev = n_sub * n_ep
    tok_spec = P(("dp", "sub", "ep"), None)
    expert_spec = P(("sub", "ep"), None, None)
    group = ("sub", "ep")
    vmem = pl.BlockSpec(memory_space=pltpu.VMEM)
    hbm = pl.BlockSpec(memory_space=pl.ANY)
    params = pltpu.CompilerParams(vmem_limit_bytes=VMEM_LIMIT)
    bf16 = jnp.bfloat16

    def shape(*dims):
        return jax.ShapeDtypeStruct(dims, bf16)

    def weights(dim, ff):
        return [
            pl.BlockSpec((dim, ff), lambda i: (0, 0)),
            pl.BlockSpec((dim, ff), lambda i: (0, 0)),
            pl.BlockSpec((ff, dim), lambda i: (0, 0)),
        ]

    def wide(x, route, gate, w_gate, w_up, w_down):
        tok, dim = x.shape
        ff = w_gate.shape[1]
        cap = min(tok, 8 * tok // n_dev)
        rows = n_dev * cap
        send, pos = pl.pallas_call(
            functools.partial(wide_pack_kernel, cap),
            out_shape=[shape(rows, dim), jax.ShapeDtypeStruct((tok, 2), jnp.int32)],
            in_specs=[vmem, vmem],
            out_specs=[vmem, vmem],
            compiler_params=params,
            name="wide_pack",
        )(route, x)
        got = lax.all_to_all(send.reshape(n_dev, cap, dim), group, 0, 0).reshape(rows, dim)
        block = pl.BlockSpec((TILE, dim), lambda i: (i, 0))
        out = pl.pallas_call(
            wide_ffn_kernel,
            out_shape=shape(rows, dim),
            grid=(rows // TILE,),
            in_specs=[block] + weights(dim, ff),
            out_specs=block,
            compiler_params=params,
            name="wide_ffn",
        )(got, w_gate, w_up, w_down)
        ret = lax.all_to_all(out.reshape(n_dev, cap, dim), group, 0, 0).reshape(rows, dim)
        return pl.pallas_call(
            wide_mix_kernel,
            out_shape=shape(tok, dim),
            in_specs=[vmem, vmem, vmem],
            out_specs=vmem,
            compiler_params=params,
            name="wide_mix",
        )(ret, pos, gate)

    cube = (SIDE, SIDE, SIDE)

    def device_step(x, route, gate, w_gate, w_up, w_down):
        tok, dim = x.shape
        ff = w_gate.shape[2]
        w_gate, w_up, w_down = w_gate[0], w_up[0], w_down[0]
        sems = pltpu.SemaphoreType.DMA
        main = pltpu.VMEM((COLORS, 2) + cube + (PART, dim), bf16)
        one_way = sems((3, COLORS, 2))
        late_in, late_out = sems((5, COLORS)), sems((5,))
        y, flag = pl.pallas_call(
            layer_kernel,
            out_shape=[shape(tok, dim), jax.ShapeDtypeStruct((1, 1), jnp.float32)],
            in_specs=[vmem, vmem, vmem, hbm, hbm, hbm],
            out_specs=[vmem, vmem],
            scratch_shapes=[
                pltpu.VMEM((dim, ff), bf16), pltpu.VMEM((dim, ff), bf16), pltpu.VMEM((ff, dim), bf16),
                main, main, main, main, main, main, main,
                pltpu.VMEM((2, COLORS) + cube + (SPARE, dim + TAIL), bf16),
                pltpu.VMEM((2, COLORS) + cube + (SPARE, dim), bf16),
                pltpu.VMEM((COLORS,) + cube + (SPARE, dim), bf16),
                pltpu.VMEM((COLORS, SIDE, SIDE, SPARE, dim), bf16),
                pltpu.VMEM((COLORS, SIDE, SPARE, dim), bf16),
                pltpu.VMEM((COLORS, 2, SIDE // 2, SIDE, SPARE, dim), bf16),
                pltpu.VMEM((COLORS, 2, SIDE, SIDE, SPARE, dim), bf16),
                pltpu.VMEM((COLORS, SIDE - 1, SIDE, SPARE, dim), bf16),
                pltpu.VMEM((COLORS, SIDE - 1, SPARE, dim), bf16),
                pltpu.VMEM((128, dim), bf16),
                pltpu.VMEM((tok, 128), jnp.float32),
                pltpu.VMEM((tok, dim), jnp.float32),
                sems((3, 2)), one_way, sems((3, 2)), one_way, late_out, late_in, late_out, late_in, sems((3,)),
            ],
            compiler_params=pltpu.CompilerParams(
                collective_id=0, has_side_effects=True, vmem_limit_bytes=67043328),
            name="layer",
        )(route.T, gate.T, x, w_gate, w_up, w_down)
        return lax.cond(flag[0, 0] > 0.0, wide, lambda *args: y, x, route, gate, w_gate, w_up, w_down)

    return jax.shard_map(
        device_step,
        mesh=mesh,
        in_specs=(tok_spec, tok_spec, tok_spec, expert_spec, expert_spec, expert_spec),
        out_specs=tok_spec,
        check_vma=False,
    )
```

```python
import functools

import jax
import jax.numpy as jnp
from jax import lax
from jax.experimental import pallas as pl
from jax.experimental.pallas import tpu as pltpu
from jax.sharding import PartitionSpec as P

MESH = pl.DeviceIdType.MESH
TILE = 256
VMEM_LIMIT = 60 * 1024 * 1024
LAYER_VMEM = 58 * 1024 * 1024
COLORS = 3
PART = 4
BASE = COLORS * PART
SPARE = 8
OVER = COLORS * SPARE
SIDE = 4
TAIL = 128


def iota(shape, dim):
    return lax.broadcasted_iota(jnp.int32, shape, dim)


def ones_where(mask):
    return jnp.where(mask, 1.0, 0.0).astype(jnp.bfloat16)


def dot(a, b):
    return jnp.dot(a, b, preferred_element_type=jnp.float32)


def expert_ffn(rows, wg_ref, wu_ref, wd_ref):
    act_a = dot(rows, wg_ref[...])
    act_b = dot(rows, wu_ref[...])
    hidden = (jax.nn.silu(act_a) * act_b).astype(jnp.bfloat16)
    return dot(hidden, wd_ref[...]).astype(jnp.bfloat16)


def ranks(route0, route1, n_experts):
    tok = route0.shape[0]
    lanes = iota((tok, n_experts), 1)
    member0 = route0 == lanes
    member1 = route1 == lanes
    lower = ones_where(iota((tok, tok), 0) >= iota((tok, tok), 1))
    rank0 = dot(lower, ones_where(member0))
    rank1 = dot(lower, ones_where(member1)) + rank0[tok - 1:tok, :]
    return member0, member1, rank0 - 1.0, rank1 - 1.0, rank1[tok - 1:tok, :]


def as_row(column):
    return jnp.transpose(jnp.broadcast_to(column, (column.shape[0], 128)))[0:1, :]


def wide_pack_kernel(cap, route_ref, x_ref, send_ref, pos_ref):
    tok = x_ref.shape[0]
    rows = send_ref.shape[0]
    member0, member1, rank0, rank1, _ = ranks(route_ref[:, 0:1], route_ref[:, 1:2], rows // cap)
    base = (iota(member0.shape, 1) * cap).astype(jnp.float32)
    pos0 = jnp.sum(jnp.where(member0, rank0 + base, 0.0), axis=1, keepdims=True)
    pos1 = jnp.sum(jnp.where(member1, rank1 + base, 0.0), axis=1, keepdims=True)
    pos_ref[...] = jnp.concatenate([pos0, pos1], axis=1).astype(jnp.int32)
    row0, row1 = as_row(pos0), as_row(pos1)

    def block(i, carry):
        place = (iota((TILE, tok), 0) + i * TILE).astype(jnp.float32)
        pick = ones_where((place == row0) | (place == row1))
        send_ref[pl.ds(pl.multiple_of(i * TILE, TILE), TILE), :] = dot(pick, x_ref[...]).astype(jnp.bfloat16)
        return carry

    lax.fori_loop(0, rows // TILE, block, 0)


def wide_ffn_kernel(x_ref, wg_ref, wu_ref, wd_ref, o_ref):
    o_ref[...] = expert_ffn(x_ref[...], wg_ref, wu_ref, wd_ref)


def wide_mix_kernel(ret_ref, pos_ref, gate_ref, y_ref):
    n_rows = ret_ref.shape[0]

    def block(i, carry):
        part = pl.ds(pl.multiple_of(i * TILE, TILE), TILE)
        lanes = iota((TILE, n_rows), 1)
        total = gate_ref[part, 0:1] * dot(ones_where(pos_ref[part, 0:1] == lanes), ret_ref[...])
        total = total + gate_ref[part, 1:2] * dot(ones_where(pos_ref[part, 1:2] == lanes), ret_ref[...])
        y_ref[part, :] = total.astype(jnp.bfloat16)
        return carry

    lax.fori_loop(0, y_ref.shape[0] // TILE, block, 0)


class Torus:
    def __init__(self):
        self.sub = lax.axis_index("sub")
        ep = lax.axis_index("ep")
        self.at = (ep % SIDE, (ep // SIDE) % SIDE, ep // (SIDE * SIDE))

    def coord(self, axis, step):
        return (self.at[axis] + step) % SIDE

    def device(self, axis, step, core=0):
        at = list(self.at)
        at[axis] = self.coord(axis, step)
        return {"sub": (self.sub + core) % 2, "ep": (at[2] * SIDE + at[1]) * SIDE + at[0]}

    def greet(self):
        barrier = pltpu.get_barrier_semaphore()
        peers = [self.device(0, 0, 1)]
        for axis in range(3):
            for step in range(1, SIDE):
                for core in range(2):
                    peers.append(self.device(axis, step, core))
        for peer in peers:
            pl.semaphore_signal(barrier, inc=1, device_id=peer, device_id_type=MESH)
        return lambda: pl.semaphore_wait(barrier, len(peers))


def remote(src, dst, send_sem, recv_sem, device):
    return pltpu.make_async_remote_copy(
        src_ref=src, dst_ref=dst, send_sem=send_sem, recv_sem=recv_sem, device_id=device, device_id_type=MESH)


def start(copies):
    for copy in copies:
        copy.start()


def drain(ref, sem):
    pltpu.make_async_copy(ref, ref, sem).wait()


def at(i, table):
    for j, steps in table.items():
        @pl.when(i == j)
        def _(steps=steps):
            for step in steps:
                step()


STEPS = (1, 3, 2)
CHUNKS = [(k, h) for h in range(2) for k in range(COLORS)]


def layer_kernel(route_ref, gate_ref, x_hbm, wg_hbm, wu_hbm, wd_hbm, y_ref, flag_ref,
                 x_ref, wg, wu, wd, a, b, c, d, cc, bb, aa, every, late, stage, sum2, sum1, relay, got3, got2, got1, last,
                 cols, total, send, recv, bsend, brecv, esend, erecv, rsend, rrecv, wsem):
    tok, dim = x_ref.shape
    rows = 2 * SIDE ** 3 * PART
    t = Torus()
    s = t.sub
    everyone_here = t.greet()
    inputs = ((x_hbm, x_ref), (wg_hbm, wg), (wu_hbm, wu), (wd_hbm, wd))
    x_load, *weights = [(src, dst, wsem.at[i]) for i, (src, dst) in enumerate(inputs)]
    for src, dst, sem in (x_load, *weights):
        pltpu.make_async_copy(src, dst, sem).start()

    def place(k):
        return tuple(t.at[(k + i) % 3] for i in range(3))

    def out(phase, k, h):
        ax, sh = (k + phase) % 3, (s + h) % 2
        c1, c2, c3 = place(k)
        copies = []
        for step in STEPS + (0,):
            to = t.coord(ax, step)
            core = h if phase == 0 else 0
            if phase == 0:
                src, dst = a.at[k, sh, to], b.at[k, s, c1]
            elif phase == 1:
                src, dst = b.at[k, sh, :, to], c.at[k, sh, c2]
            else:
                src, dst = c.at[k, sh, :, :, to], d.at[k, sh, c3]
            if step == 0 and core == 0:
                copies.append(pltpu.make_async_copy(src, dst, recv.at[phase, k, h]))
            else:
                copies.append(remote(src, dst, send.at[phase, h], recv.at[phase, k, h], t.device(ax, step, core)))
        return copies

    def back(phase, k, h):
        ax, sh = (k + phase) % 3, (s + h) % 2
        c1, c2, c3 = place(k)
        copies = []
        for step in STEPS + (0,):
            to = t.coord(ax, step)
            core = h if phase == 0 else 0
            if phase == 0:
                src, dst = bb.at[k, sh, to], aa.at[k, s, c1]
            elif phase == 1:
                src, dst = cc.at[k, sh, to], bb.at[k, sh, :, c2]
            else:
                src, dst = d.at[k, sh, to], cc.at[k, sh, :, :, c3]
            if step == 0 and core == 0:
                copies.append(pltpu.make_async_copy(src, dst, brecv.at[phase, k, h]))
            else:
                copies.append(remote(src, dst, bsend.at[phase, h], brecv.at[phase, k, h], t.device(ax, step, core)))
        return copies

    def gather(phase, k):
        c1, c2, c3 = place(k)
        if phase == 3:
            part = every.at[s, k]
            return [remote(part, part, esend.at[3], erecv.at[3, k], t.device(0, 0, 1))]
        if phase == 4:
            copies = []
            for step, part in ((1, slice(0, SIDE // 2)), (3, slice(SIDE // 2, SIDE))):
                far = every.at[s, k, part, :, t.coord((k + 2) % 3, -step)]
                copies.append(remote(far, far, esend.at[4], erecv.at[4, k], t.device((k + 2) % 3, step)))
            return copies
        mine = (every.at[s, k, c1, c2, c3], every.at[s, k, :, c2, c3], every.at[s, k, :, :, c3])[phase]
        return [remote(mine, mine, esend.at[phase], erecv.at[phase, k], t.device((k + phase) % 3, step))
                for step in (STEPS[:2] if phase == 2 else STEPS)]

    def gathered(k):
        return (every.at[0, k, 0:3, 0, 0], every.at[0, k, 0:3, :, 0], every.at[0, k, 0:2], every.at[0, k],
                every.at[0, k, 0:1])

    def reduce(phase, k):
        if phase == 3:
            return [remote(late.at[1 - s, k], stage.at[k], rsend.at[3], rrecv.at[3, k], t.device(0, 0, 1))]
        copies = []
        if phase == 4:
            far = t.coord((k + 2) % 3, 2)
            for i, (step, part) in enumerate(((1, slice(0, SIDE // 2)), (3, slice(SIDE // 2, SIDE)))):
                copies.append(remote(late.at[s, k, part, :, far], relay.at[k, i], rsend.at[4],
                                     rrecv.at[4, k], t.device((k + 2) % 3, step)))
            return copies
        for step in STEPS[:2] if phase == 2 else STEPS:
            to = t.coord((k + phase) % 3, step)
            src = (sum1.at[k, to], sum2.at[k, :, to], late.at[s, k, :, :, to])[phase]
            dst = (got1, got2, got3)[phase].at[k, step // 2 if phase == 2 else step - 1]
            copies.append(remote(src, dst, rsend.at[phase], rrecv.at[phase, k], t.device((k + phase) % 3, step)))
        return copies

    def merge(phase, k):
        if phase == 3:
            def add(i, carry):
                late[s, k, i] = late[s, k, i] + stage[k, i]
                return carry

            lax.fori_loop(0, SIDE, add, 0)
            return
        if phase == 4:
            right, left = t.coord((k + 2) % 3, 1), t.coord((k + 2) % 3, 3)
            late[s, k, 0:SIDE // 2, :, right] = late[s, k, 0:SIDE // 2, :, right] + relay[k, 0]
            late[s, k, SIDE // 2:SIDE, :, left] = late[s, k, SIDE // 2:SIDE, :, left] + relay[k, 1]
            return
        mine = t.at[(k + phase) % 3]
        got = (got1, got2, got3)[phase]
        more = got[k, 0] + got[k, 1]
        if phase < 2:
            more = more + got[k, 2]
        if phase == 2:
            sum2[k] = late[s, k, :, :, mine] + more
        elif phase == 1:
            sum1[k] = sum2[k, :, mine] + more
        else:
            last[k * SPARE:(k + 1) * SPARE, :] = sum1[k, mine] + more

    n_experts = 2 * SIDE ** 3
    table = jnp.concatenate([route_ref[...].astype(jnp.float32), gate_ref[...], jnp.zeros((4, tok), jnp.float32)], axis=0)
    table = jnp.transpose(table)
    route0, route1 = table[:, 0:1].astype(jnp.int32), table[:, 1:2].astype(jnp.int32)
    gates = slice(2, 4)
    cols[:, gates] = table[:, gates]
    member0, member1, rank0, rank1, count = ranks(route0, route1, n_experts)
    lanes = iota((1, n_experts), 1)
    sub, ep = lanes // (SIDE ** 3), lanes % (SIDE ** 3)
    axes = (ep % SIDE, (ep // SIDE) % SIDE, ep // (SIDE * SIDE))
    first = []
    for k in range(COLORS):
        d1, d2, d3 = (axes[(k + i) % 3] for i in range(3))
        block = ((sub * SIDE + d1) * SIDE + d2) * SIDE + d3
        first.append((k * rows + block * PART - k * PART).astype(jnp.float32))
    excess = jnp.maximum(count - BASE, 0.0)
    strict = ones_where(iota((n_experts, n_experts), 0) < iota((n_experts, n_experts), 1))
    ahead = dot(jnp.broadcast_to(excess, (8, n_experts)).astype(jnp.bfloat16), strict)[0:1, :]
    n_over = jnp.sum(excess, axis=1, keepdims=True)
    nowhere = 4.0 * COLORS * rows

    def places(member, rank):
        base = jnp.where(rank < PART, first[0], jnp.where(rank < 2 * PART, first[1], first[2]))
        behind = ahead + (rank - BASE)
        where = jnp.where(rank < BASE, base + rank, jnp.where(behind < OVER, COLORS * rows + behind, nowhere))
        return jnp.sum(jnp.where(member, where, 0.0), axis=1, keepdims=True)

    pos0, pos1 = places(member0, rank0), places(member1, rank1)
    cols[:, 0:1] = pos0
    cols[:, 1:2] = pos1
    both = jnp.transpose(jnp.where(iota((tok, 128), 1) == 0, pos0, pos1))
    row0, row1 = both[0:1, :], both[1:2, :]

    def relay_gather(phase, k):
        drain(gathered(k)[phase], erecv.at[phase, k])
        start(gather({0: 1, 1: 2, 2: 4, 4: 3}[phase], k))

    def relay_out(phase, k, h):
        drain(d.at[k, 0], recv.at[phase, k, h])
        start(out(phase + 1, k, h))

    def relay_back(phase, k, h):
        drain(d.at[k, 0], brecv.at[phase, k, h])
        start(back(phase - 1, k, h))

    def relay_reduce(phase, k):
        drain((got1, got2, got3, stage, relay)[phase].at[k], rrecv.at[phase, k])
        merge(phase, k)
        if phase:
            start(reduce({3: 4, 4: 2, 2: 1, 1: 0}[phase], k))

    firsts, seconds = CHUNKS[:COLORS], CHUNKS[COLORS:]

    def pack_over():
        spot = (iota((32, tok), 0) + COLORS * rows).astype(jnp.float32)
        pick0, pick1 = ones_where(spot == row0), ones_where(spot == row1)
        got = dot(pick0 + pick1, x_ref[...]).astype(jnp.bfloat16)
        expert0 = jnp.broadcast_to(route0 + 1, (tok, TAIL)).astype(jnp.bfloat16)
        expert1 = jnp.broadcast_to(route1 + 1, (tok, TAIL)).astype(jnp.bfloat16)
        owner = dot(pick0, expert0) + dot(pick1, expert1)
        flag = jnp.where(n_over > OVER, 1.0, 0.0)
        tail = jnp.where(iota((32, TAIL), 1) == 0, owner, flag).astype(jnp.bfloat16)
        for k in range(COLORS):
            c1, c2, c3 = place(k)
            part = slice(k * SPARE, (k + 1) * SPARE)
            every[s, k, c1, c2, c3, :, 0:dim] = got[part, :]
            every[s, k, c1, c2, c3, :, dim:dim + TAIL] = tail[part, :]

    def pack(i, carry):
        k, sh = i % COLORS, (s + i // COLORS) % 2
        spot = (iota((TILE, tok), 0) + (k * rows + sh * TILE)).astype(jnp.float32)
        pick = ones_where((spot == row0) | (spot == row1))
        got = dot(pick, x_ref[...]).astype(jnp.bfloat16)
        a[k, sh] = got.reshape(SIDE, SIDE, SIDE, PART, dim)
        events = {j + 1: [lambda q=q: start(out(0, *q))] for j, q in enumerate(firsts)}
        events[1] = [everyone_here] + [lambda k=k: start(gather(0, k)) for k in range(COLORS)] + events[1]
        at(i, events)
        return carry

    pltpu.make_async_copy(*x_load).wait()
    pack_over()
    lax.fori_loop(0, len(CHUNKS), pack, 0)
    for k in range(COLORS):
        relay_gather(0, k)
    for q in seconds:
        start(out(0, *q))
    for k in range(COLORS):
        relay_gather(1, k)
    for q in firsts:
        relay_out(0, *q)
    for k in range(COLORS):
        relay_gather(2, k)
    for q in seconds:
        relay_out(0, *q)
    for q in firsts:
        relay_out(1, *q)
    for src, dst, sem in weights:
        pltpu.make_async_copy(src, dst, sem).wait()
    me = (s * SIDE ** 3 + lax.axis_index("ep") + 1).astype(jnp.float32)
    flag_ref[...] = jnp.zeros_like(flag_ref)

    over_steps, main_steps = (0, 1, 2, 3, 4, 8), (5, 6, 7, 9, 10, 11)
    before = {j: [lambda q=q: drain(d.at[q[0], 0], recv.at[2, q[0], q[1]])] for j, q in zip(main_steps, CHUNKS)}
    before.update({over_steps[COLORS + k]: [lambda k=k: drain(gathered(k)[3], erecv.at[3, k])] for k in range(COLORS)})
    before[0] = [lambda k=k: relay_gather(4, k) for k in range(COLORS)]
    before[4].insert(0, lambda: start(reduce(3, 0)))
    before[5].insert(0, lambda: start(reduce(3, 1)))
    before[9].insert(0, lambda: start(reduce(3, 2)))
    after = {j: [lambda q=q: start(back(2, *q))] for j, q in zip(main_steps, CHUNKS)}
    after[2] = [lambda q=q: relay_out(1, *q) for q in seconds]
    after[6].append(lambda: relay_reduce(3, 0))
    after[9].append(lambda: relay_reduce(3, 1))
    after[11].append(lambda: relay_reduce(3, 2))

    def work(i, carry):
        at(i, before)
        is_over = (i < 5) | (i == 8)

        @pl.when(is_over)
        def _():
            j = jnp.where(i == 8, 5, i)
            core, k = (s + j // COLORS) % 2, j % COLORS
            got = every[core, k].reshape(2 * TILE, dim + TAIL)
            tail = got[:, dim:dim + TAIL].astype(jnp.float32)
            flag_ref[...] = jnp.maximum(flag_ref[...], jnp.max(tail[:, 1:2], axis=0, keepdims=True))
            result = expert_ffn(got[:, 0:dim], wg, wu, wd).astype(jnp.float32)
            result = jnp.where(tail[:, 0:1] == me, result, 0.0).astype(jnp.bfloat16)
            late[core, k] = result.reshape(SIDE, SIDE, SIDE, SPARE, dim)

        @pl.when(jnp.logical_not(is_over))
        def _():
            j = jnp.where(i < 8, i - 5, i - 6)
            k, sh = j % COLORS, (s + j // COLORS) % 2
            d[k, sh] = expert_ffn(d[k, sh].reshape(TILE, dim), wg, wu, wd).reshape(SIDE, SIDE, SIDE, PART, dim)

        at(i, after)
        return carry

    lax.fori_loop(0, 12, work, 0)
    for q in firsts:
        relay_back(2, *q)
    for k in range(COLORS):
        relay_reduce(4, k)
    for q in seconds:
        relay_back(2, *q)
    for k in range(COLORS):
        relay_reduce(2, k)
    for q in firsts:
        relay_back(1, *q)
    for k in range(COLORS):
        relay_reduce(1, k)
    for q in seconds:
        relay_back(1, *q)
    last[...] = jnp.zeros_like(last)
    for k in range(COLORS):
        relay_reduce(0, k)
    lanes = (iota((TILE, last.shape[0]), 1) + COLORS * rows).astype(jnp.float32)
    for part in range(tok // TILE):
        where = pl.ds(part * TILE, TILE)
        add = cols[where, 2:3] * dot(ones_where(cols[where, 0:1] == lanes), last[...])
        total[where, :] = add + cols[where, 3:4] * dot(ones_where(cols[where, 1:2] == lanes), last[...])

    def mix(i, final=False):
        k, sh = i % COLORS, (s + i // COLORS) % 2
        got = aa[k, sh].reshape(TILE, dim)
        lanes = (iota((TILE, TILE), 1) + (k * rows + sh * TILE)).astype(jnp.float32)
        for part in range(tok // TILE):
            where = pl.ds(part * TILE, TILE)
            add = cols[where, 2:3] * dot(ones_where(cols[where, 0:1] == lanes), got)
            add = add + cols[where, 3:4] * dot(ones_where(cols[where, 1:2] == lanes), got)
            if final:
                y_ref[where, :] = (total[where, :] + add).astype(jnp.bfloat16)
            else:
                total[where, :] += add

    def mix_early(i, carry):
        at(i, {j: [lambda q=q: drain(d.at[q[0], 0], brecv.at[0, q[0], q[1]])] for j, q in enumerate(CHUNKS)})
        mix(i)
        return carry

    lax.fori_loop(0, len(CHUNKS) - 1, mix_early, 0)
    drain(d.at[0, 0], brecv.at[0, CHUNKS[-1][0], CHUNKS[-1][1]])
    mix(len(CHUNKS) - 1, final=True)
    for phase in range(3):
        for h in range(2):
            sent = d.at[:, 0] if phase == 0 and h else d.at[:, 0, 0:3]
            drain(sent, send.at[phase, h])
            drain(sent, bsend.at[phase, h])
    for phase in range(5):
        drain(gathered(slice(None))[phase], esend.at[phase])
        drain((got1, got2, got3, stage, relay)[phase], rsend.at[phase])


def solution(mesh):
    n_sub, n_ep = mesh.shape["sub"], mesh.shape["ep"]
    n_dev = n_sub * n_ep
    tok_spec = P(("dp", "sub", "ep"), None)
    expert_spec = P(("sub", "ep"), None, None)
    group = ("sub", "ep")
    vmem = pl.BlockSpec(memory_space=pltpu.VMEM)
    hbm = pl.BlockSpec(memory_space=pl.ANY)
    params = pltpu.CompilerParams(vmem_limit_bytes=VMEM_LIMIT)
    bf16 = jnp.bfloat16

    def shape(*dims):
        return jax.ShapeDtypeStruct(dims, bf16)

    def weights(dim, ff):
        return [
            pl.BlockSpec((dim, ff), lambda i: (0, 0)),
            pl.BlockSpec((dim, ff), lambda i: (0, 0)),
            pl.BlockSpec((ff, dim), lambda i: (0, 0)),
        ]

    def wide(x, route, gate, w_gate, w_up, w_down):
        tok, dim = x.shape
        ff = w_gate.shape[1]
        cap = min(tok, 8 * tok // n_dev)
        rows = n_dev * cap
        send, pos = pl.pallas_call(
            functools.partial(wide_pack_kernel, cap),
            out_shape=[shape(rows, dim), jax.ShapeDtypeStruct((tok, 2), jnp.int32)],
            in_specs=[vmem, vmem],
            out_specs=[vmem, vmem],
            compiler_params=params,
            name="wide_pack",
        )(route, x)
        got = lax.all_to_all(send.reshape(n_dev, cap, dim), group, 0, 0).reshape(rows, dim)
        block = pl.BlockSpec((TILE, dim), lambda i: (i, 0))
        out = pl.pallas_call(
            wide_ffn_kernel,
            out_shape=shape(rows, dim),
            grid=(rows // TILE,),
            in_specs=[block] + weights(dim, ff),
            out_specs=block,
            compiler_params=params,
            name="wide_ffn",
        )(got, w_gate, w_up, w_down)
        ret = lax.all_to_all(out.reshape(n_dev, cap, dim), group, 0, 0).reshape(rows, dim)
        return pl.pallas_call(
            wide_mix_kernel,
            out_shape=shape(tok, dim),
            in_specs=[vmem, vmem, vmem],
            out_specs=vmem,
            compiler_params=params,
            name="wide_mix",
        )(ret, pos, gate)

    cube = (SIDE, SIDE, SIDE)

    def device_step(x, route, gate, w_gate, w_up, w_down):
        tok, dim = x.shape
        ff = w_gate.shape[2]
        w_gate, w_up, w_down = w_gate[0], w_up[0], w_down[0]
        sems = pltpu.SemaphoreType.DMA
        main = pltpu.VMEM((COLORS, 2) + cube + (PART, dim), bf16)
        one_way = sems((3, COLORS, 2))
        late_in, late_out = sems((5, COLORS)), sems((5,))
        y, flag = pl.pallas_call(
            layer_kernel,
            out_shape=[pltpu.VMEM((tok, dim), bf16), jax.ShapeDtypeStruct((1, 1), jnp.float32)],
            in_specs=[vmem, vmem, hbm, hbm, hbm, hbm],
            out_specs=[vmem, vmem],
            scratch_shapes=[
                pltpu.VMEM((tok, dim), bf16),
                pltpu.VMEM((dim, ff), bf16), pltpu.VMEM((dim, ff), bf16), pltpu.VMEM((ff, dim), bf16),
                main, main, main, main, main, main, main,
                pltpu.VMEM((2, COLORS) + cube + (SPARE, dim + TAIL), bf16),
                pltpu.VMEM((2, COLORS) + cube + (SPARE, dim), bf16),
                pltpu.VMEM((COLORS,) + cube + (SPARE, dim), bf16),
                pltpu.VMEM((COLORS, SIDE, SIDE, SPARE, dim), bf16),
                pltpu.VMEM((COLORS, SIDE, SPARE, dim), bf16),
                pltpu.VMEM((COLORS, 2, SIDE // 2, SIDE, SPARE, dim), bf16),
                pltpu.VMEM((COLORS, 2, SIDE, SIDE, SPARE, dim), bf16),
                pltpu.VMEM((COLORS, SIDE - 1, SIDE, SPARE, dim), bf16),
                pltpu.VMEM((COLORS, SIDE - 1, SPARE, dim), bf16),
                pltpu.VMEM((128, dim), bf16),
                pltpu.VMEM((tok, 128), jnp.float32),
                pltpu.VMEM((tok, dim), jnp.float32),
                sems((3, 2)), one_way, sems((3, 2)), one_way, late_out, late_in, late_out, late_in, sems((4,)),
            ],
            compiler_params=pltpu.CompilerParams(
                collective_id=0, has_side_effects=True, vmem_limit_bytes=LAYER_VMEM),
            name="layer",
        )(route.T, gate.T, x, w_gate, w_up, w_down)
        return lax.cond(flag[0, 0] > 0.0, wide, lambda *args: y, x, route, gate, w_gate, w_up, w_down)

    return jax.shard_map(
        device_step,
        mesh=mesh,
        in_specs=(tok_spec, tok_spec, tok_spec, expert_spec, expert_spec, expert_spec),
        out_specs=tok_spec,
        check_vma=False,
    )
```

```python
import functools

import jax
import jax.numpy as jnp
from jax import lax
from jax.experimental import pallas as pl
from jax.experimental.pallas import tpu as pltpu
from jax.sharding import PartitionSpec as P

MESH = pl.DeviceIdType.MESH
TILE = 256
VMEM_LIMIT = 60 * 1024 * 1024
LAYER_VMEM = 58 * 1024 * 1024
COLORS = 3
PART = 4
BASE = COLORS * PART
SPARE = 8
OVER = COLORS * SPARE
SIDE = 4
TAIL = 128


def iota(shape, dim):
    return lax.broadcasted_iota(jnp.int32, shape, dim)


def ones_where(mask):
    return jnp.where(mask, 1.0, 0.0).astype(jnp.bfloat16)


def dot(a, b):
    return jnp.dot(a, b, preferred_element_type=jnp.float32)


def expert_ffn(rows, wg_ref, wu_ref, wd_ref):
    act_a = dot(rows, wg_ref[...])
    act_b = dot(rows, wu_ref[...])
    hidden = (jax.nn.silu(act_a) * act_b).astype(jnp.bfloat16)
    return dot(hidden, wd_ref[...]).astype(jnp.bfloat16)


def ranks(route0, route1, n_experts):
    tok = route0.shape[0]
    lanes = iota((tok, n_experts), 1)
    member0 = route0 == lanes
    member1 = route1 == lanes
    lower = ones_where(iota((tok, tok), 0) >= iota((tok, tok), 1))
    rank0 = dot(lower, ones_where(member0))
    rank1 = dot(lower, ones_where(member1)) + rank0[tok - 1:tok, :]
    return member0, member1, rank0 - 1.0, rank1 - 1.0, rank1[tok - 1:tok, :]


def as_row(column):
    return jnp.transpose(jnp.broadcast_to(column, (column.shape[0], 128)))[0:1, :]


def wide_pack_kernel(cap, route_ref, x_ref, send_ref, pos_ref):
    tok = x_ref.shape[0]
    rows = send_ref.shape[0]
    member0, member1, rank0, rank1, _ = ranks(route_ref[:, 0:1], route_ref[:, 1:2], rows // cap)
    base = (iota(member0.shape, 1) * cap).astype(jnp.float32)
    pos0 = jnp.sum(jnp.where(member0, rank0 + base, 0.0), axis=1, keepdims=True)
    pos1 = jnp.sum(jnp.where(member1, rank1 + base, 0.0), axis=1, keepdims=True)
    pos_ref[...] = jnp.concatenate([pos0, pos1], axis=1).astype(jnp.int32)
    row0, row1 = as_row(pos0), as_row(pos1)

    def block(i, carry):
        place = (iota((TILE, tok), 0) + i * TILE).astype(jnp.float32)
        pick = ones_where((place == row0) | (place == row1))
        send_ref[pl.ds(pl.multiple_of(i * TILE, TILE), TILE), :] = dot(pick, x_ref[...]).astype(jnp.bfloat16)
        return carry

    lax.fori_loop(0, rows // TILE, block, 0)


def wide_ffn_kernel(x_ref, wg_ref, wu_ref, wd_ref, o_ref):
    o_ref[...] = expert_ffn(x_ref[...], wg_ref, wu_ref, wd_ref)


def wide_mix_kernel(ret_ref, pos_ref, gate_ref, y_ref):
    n_rows = ret_ref.shape[0]

    def block(i, carry):
        part = pl.ds(pl.multiple_of(i * TILE, TILE), TILE)
        lanes = iota((TILE, n_rows), 1)
        total = gate_ref[part, 0:1] * dot(ones_where(pos_ref[part, 0:1] == lanes), ret_ref[...])
        total = total + gate_ref[part, 1:2] * dot(ones_where(pos_ref[part, 1:2] == lanes), ret_ref[...])
        y_ref[part, :] = total.astype(jnp.bfloat16)
        return carry

    lax.fori_loop(0, y_ref.shape[0] // TILE, block, 0)


class Torus:
    def __init__(self):
        self.sub = lax.axis_index("sub")
        ep = lax.axis_index("ep")
        self.at = (ep % SIDE, (ep // SIDE) % SIDE, ep // (SIDE * SIDE))

    def coord(self, axis, step):
        return (self.at[axis] + step) % SIDE

    def device(self, axis, step, core=0):
        at = list(self.at)
        at[axis] = self.coord(axis, step)
        return {"sub": (self.sub + core) % 2, "ep": (at[2] * SIDE + at[1]) * SIDE + at[0]}

    def greet(self):
        barrier = pltpu.get_barrier_semaphore()
        peers = [self.device(0, 0, 1)]
        for axis in range(3):
            for step in range(1, SIDE):
                for core in range(2):
                    peers.append(self.device(axis, step, core))
        for peer in peers:
            pl.semaphore_signal(barrier, inc=1, device_id=peer, device_id_type=MESH)
        return lambda: pl.semaphore_wait(barrier, len(peers))


def remote(src, dst, send_sem, recv_sem, device):
    return pltpu.make_async_remote_copy(
        src_ref=src, dst_ref=dst, send_sem=send_sem, recv_sem=recv_sem, device_id=device, device_id_type=MESH)


class Stay:
    def __init__(self, src, dst):
        self.src, self.dst = src, dst

    def start(self):
        self.dst[...] = self.src[...]


def start(copies):
    for copy in copies:
        copy.start()


def drain(ref, sem):
    pltpu.make_async_copy(ref, ref, sem).wait()


def at(i, table):
    for j, steps in table.items():
        @pl.when(i == j)
        def _(steps=steps):
            for step in steps:
                step()


STEPS = (1, 3, 2)
CHUNKS = [(k, h) for h in range(2) for k in range(COLORS)]


def layer_kernel(route_ref, gate_ref, x_hbm, wg_hbm, wu_hbm, wd_hbm, y_ref, flag_ref,
                 x_ref, wg, wu, wd, a, b, c, d, cc, bb, aa, every, note, late, stage, sum2, sum1, relay, got3, got2, got1, last,
                 cols, total, send, recv, bsend, brecv, esend, erecv, rsend, rrecv, nsend, nrecv, wsem):
    tok, dim = x_ref.shape
    rows = 2 * SIDE ** 3 * PART
    t = Torus()
    s = t.sub
    everyone_here = t.greet()
    inputs = ((x_hbm, x_ref), (wg_hbm, wg), (wu_hbm, wu), (wd_hbm, wd))
    x_load, *weights = [(src, dst, wsem.at[i]) for i, (src, dst) in enumerate(inputs)]
    for src, dst, sem in (x_load, *weights):
        pltpu.make_async_copy(src, dst, sem).start()

    def place(k):
        return tuple(t.at[(k + i) % 3] for i in range(3))

    def out(phase, k, h):
        ax, sh = (k + phase) % 3, (s + h) % 2
        c1, c2, c3 = place(k)
        copies = []
        for step in STEPS + (0,):
            to = t.coord(ax, step)
            core = h if phase == 0 else 0
            if phase == 0:
                src, dst = a.at[k, sh, to], b.at[k, s, c1]
            elif phase == 1:
                src, dst = b.at[k, sh, :, to], c.at[k, sh, c2]
            else:
                src, dst = c.at[k, sh, :, :, to], d.at[k, sh, c3]
            if step == 0 and core == 0:
                copies.append(Stay(src, dst))
            else:
                copies.append(remote(src, dst, send.at[phase, h], recv.at[phase, k, h], t.device(ax, step, core)))
        return copies

    def back(phase, k, h):
        ax, sh = (k + phase) % 3, (s + h) % 2
        c1, c2, c3 = place(k)
        copies = []
        for step in STEPS + (0,):
            to = t.coord(ax, step)
            core = h if phase == 0 else 0
            if phase == 0:
                src, dst = bb.at[k, sh, to], aa.at[k, s, c1]
            elif phase == 1:
                src, dst = cc.at[k, sh, to], bb.at[k, sh, :, c2]
            else:
                src, dst = d.at[k, sh, to], cc.at[k, sh, :, :, c3]
            if step == 0 and core == 0:
                copies.append(Stay(src, dst))
            else:
                copies.append(remote(src, dst, bsend.at[phase, h], brecv.at[phase, k, h], t.device(ax, step, core)))
        return copies

    def spread(rows_of, phase, k, send_sem, recv_sem):
        c1, c2, c3 = place(k)
        ax = (k + min(phase, 2)) % 3
        if phase == 3:
            part = rows_of.at[s, k]
            return [remote(part, part, send_sem, recv_sem, t.device(0, 0, 1))]
        if phase == 4:
            ax, copies = (k + 2) % 3, []
            for step, part in ((1, slice(0, SIDE // 2)), (3, slice(SIDE // 2, SIDE))):
                far = rows_of.at[s, k, part, :, t.coord(ax, -step)]
                copies.append(remote(far, far, send_sem, recv_sem, t.device(ax, step)))
            return copies
        mine = (rows_of.at[s, k, c1, c2, c3], rows_of.at[s, k, :, c2, c3], rows_of.at[s, k, :, :, c3])[phase]
        return [remote(mine, mine, send_sem, recv_sem, t.device(ax, step))
                for step in (STEPS[:2] if phase == 2 else STEPS)]

    def gather(phase, k):
        copies = spread(every, phase, k, esend.at[phase], erecv.at[phase, k])
        if k == 0:
            copies = spread(note, phase, 0, nsend.at[phase], nrecv.at[phase]) + copies
        return copies

    def gathered(rows_of, k):
        return (rows_of.at[0, k, 0:3, 0, 0], rows_of.at[0, k, 0:3, :, 0], rows_of.at[0, k, 0:2], rows_of.at[0, k],
                rows_of.at[0, k, 0:1])

    def await_gather(phase, k):
        drain(gathered(every, k)[phase], erecv.at[phase, k])
        if k == 0:
            drain(gathered(note, 0)[phase], nrecv.at[phase])

    def turn_note(core):
        for i in range(SIDE):
            note[core, 1, :, :, i] = note[core, 0, i]
            note[core, 2, i] = note[core, 0, :, :, i]

    def reduce(phase, k):
        if phase == 3:
            return [remote(late.at[1 - s, k], stage.at[k], rsend.at[3], rrecv.at[3, k], t.device(0, 0, 1))]
        copies = []
        if phase == 4:
            far = t.coord((k + 2) % 3, 2)
            for i, (step, part) in enumerate(((1, slice(0, SIDE // 2)), (3, slice(SIDE // 2, SIDE)))):
                copies.append(remote(late.at[s, k, part, :, far], relay.at[k, i], rsend.at[4],
                                     rrecv.at[4, k], t.device((k + 2) % 3, step)))
            return copies
        for step in STEPS[:2] if phase == 2 else STEPS:
            to = t.coord((k + phase) % 3, step)
            src = (sum1.at[k, to], sum2.at[k, :, to], late.at[s, k, :, :, to])[phase]
            dst = (got1, got2, got3)[phase].at[k, step // 2 if phase == 2 else step - 1]
            copies.append(remote(src, dst, rsend.at[phase], rrecv.at[phase, k], t.device((k + phase) % 3, step)))
        return copies

    def merge(phase, k):
        if phase == 3:
            def add(i, carry):
                late[s, k, i] = late[s, k, i] + stage[k, i]
                return carry

            lax.fori_loop(0, SIDE, add, 0)
            return
        if phase == 4:
            right, left = t.coord((k + 2) % 3, 1), t.coord((k + 2) % 3, 3)
            late[s, k, 0:SIDE // 2, :, right] = late[s, k, 0:SIDE // 2, :, right] + relay[k, 0]
            late[s, k, SIDE // 2:SIDE, :, left] = late[s, k, SIDE // 2:SIDE, :, left] + relay[k, 1]
            return
        mine = t.at[(k + phase) % 3]
        got = (got1, got2, got3)[phase]
        more = got[k, 0] + got[k, 1]
        if phase < 2:
            more = more + got[k, 2]
        if phase == 2:
            sum2[k] = late[s, k, :, :, mine] + more
        elif phase == 1:
            sum1[k] = sum2[k, :, mine] + more
        else:
            last[k * SPARE:(k + 1) * SPARE, :] = sum1[k, mine] + more

    n_experts = 2 * SIDE ** 3
    table = jnp.concatenate([route_ref[...].astype(jnp.float32), gate_ref[...], jnp.zeros((4, tok), jnp.float32)], axis=0)
    table = jnp.transpose(table)
    route0, route1 = table[:, 0:1].astype(jnp.int32), table[:, 1:2].astype(jnp.int32)
    gates = slice(2, 4)
    cols[:, gates] = table[:, gates]
    member0, member1, rank0, rank1, count = ranks(route0, route1, n_experts)
    lanes = iota((1, n_experts), 1)
    sub, ep = lanes // (SIDE ** 3), lanes % (SIDE ** 3)
    axes = (ep % SIDE, (ep // SIDE) % SIDE, ep // (SIDE * SIDE))
    first = []
    for k in range(COLORS):
        d1, d2, d3 = (axes[(k + i) % 3] for i in range(3))
        block = ((sub * SIDE + d1) * SIDE + d2) * SIDE + d3
        first.append((k * rows + block * PART - k * PART).astype(jnp.float32))
    excess = jnp.maximum(count - BASE, 0.0)
    strict = ones_where(iota((n_experts, n_experts), 0) < iota((n_experts, n_experts), 1))
    ahead = dot(jnp.broadcast_to(excess, (8, n_experts)).astype(jnp.bfloat16), strict)[0:1, :]
    n_over = jnp.sum(excess, axis=1, keepdims=True)
    nowhere = 4.0 * COLORS * rows

    def places(member, rank):
        base = jnp.where(rank < PART, first[0], jnp.where(rank < 2 * PART, first[1], first[2]))
        behind = ahead + (rank - BASE)
        where = jnp.where(rank < BASE, base + rank, jnp.where(behind < OVER, COLORS * rows + behind, nowhere))
        return jnp.sum(jnp.where(member, where, 0.0), axis=1, keepdims=True)

    pos0, pos1 = places(member0, rank0), places(member1, rank1)
    cols[:, 0:1] = pos0
    cols[:, 1:2] = pos1
    both = jnp.transpose(jnp.where(iota((tok, 128), 1) == 0, pos0, pos1))
    row0, row1 = both[0:1, :], both[1:2, :]

    def relay_gather(phase, k):
        await_gather(phase, k)
        start(gather({0: 1, 1: 2, 2: 4, 4: 3}[phase], k))

    def brought(phase, k, h):
        return d.at[k, 0] if phase == 0 and h else d.at[k, 0, 0:3]

    def relay_out(phase, k, h):
        drain(brought(phase, k, h), recv.at[phase, k, h])
        start(out(phase + 1, k, h))

    def relay_back(phase, k, h):
        drain(brought(phase, k, h), brecv.at[phase, k, h])
        start(back(phase - 1, k, h))

    def relay_reduce(phase, k):
        drain((got1, got2, got3, stage, relay)[phase].at[k], rrecv.at[phase, k])
        merge(phase, k)
        if phase:
            start(reduce({3: 4, 4: 2, 2: 1, 1: 0}[phase], k))

    firsts, seconds = CHUNKS[:COLORS], CHUNKS[COLORS:]

    def pack_over():
        spot = (iota((32, tok), 0) + COLORS * rows).astype(jnp.float32)
        pick0, pick1 = ones_where(spot == row0), ones_where(spot == row1)
        got = dot(pick0 + pick1, x_ref[...]).astype(jnp.bfloat16)
        expert0 = jnp.broadcast_to(route0 + 1, (tok, TAIL)).astype(jnp.bfloat16)
        expert1 = jnp.broadcast_to(route1 + 1, (tok, TAIL)).astype(jnp.bfloat16)
        owner = dot(pick0, expert0) + dot(pick1, expert1)
        lane = iota((SPARE, TAIL), 1)
        mark = jnp.where(lane == COLORS, jnp.where(n_over > OVER, 1.0, 0.0), 0.0)
        for k in range(COLORS):
            c1, c2, c3 = place(k)
            part = slice(k * SPARE, (k + 1) * SPARE)
            every[s, k, c1, c2, c3] = got[part, :]
            mark = jnp.where(lane == k, owner[part, :], mark)
        note[s, 0, t.at[0], t.at[1], t.at[2]] = mark.astype(jnp.bfloat16)

    def pack(i, carry):
        k, sh = i % COLORS, (s + i // COLORS) % 2
        spot = (iota((TILE, tok), 0) + (k * rows + sh * TILE)).astype(jnp.float32)
        pick = ones_where((spot == row0) | (spot == row1))
        got = dot(pick, x_ref[...]).astype(jnp.bfloat16)
        a[k, sh] = got.reshape(SIDE, SIDE, SIDE, PART, dim)
        events = {j + 1: [lambda q=q: start(out(0, *q))] for j, q in enumerate(firsts)}
        events[1] = [everyone_here] + [lambda k=k: start(gather(0, k)) for k in range(COLORS)] + events[1]
        at(i, events)
        return carry

    pltpu.make_async_copy(*x_load).wait()
    pack_over()
    lax.fori_loop(0, len(CHUNKS), pack, 0)
    for k in range(COLORS):
        relay_gather(0, k)
    for q in seconds:
        start(out(0, *q))
    for k in range(COLORS):
        relay_gather(1, k)
    for q in firsts:
        relay_out(0, *q)
    for k in range(COLORS):
        relay_gather(2, k)
    for q in seconds:
        relay_out(0, *q)
    for q in firsts:
        relay_out(1, *q)
    for src, dst, sem in weights:
        pltpu.make_async_copy(src, dst, sem).wait()
    me = (s * SIDE ** 3 + lax.axis_index("ep") + 1).astype(jnp.float32)
    flag_ref[...] = jnp.zeros_like(flag_ref)

    over_steps, main_steps = (0, 1, 2, 3, 4, 8), (5, 6, 7, 9, 10, 11)
    before = {j: [lambda q=q: drain(brought(2, *q), recv.at[2, q[0], q[1]])] for j, q in zip(main_steps, CHUNKS)}
    before.update({over_steps[COLORS + k]: [lambda k=k: await_gather(3, k)] for k in range(COLORS)})
    before[0] = [lambda k=k: relay_gather(4, k) for k in range(COLORS)]
    before[0].append(lambda: turn_note(s))
    before[over_steps[COLORS]].append(lambda: turn_note(1 - s))
    before[4].insert(0, lambda: start(reduce(3, 0)))
    before[5].insert(0, lambda: start(reduce(3, 1)))
    before[9].insert(0, lambda: start(reduce(3, 2)))
    after = {j: [lambda q=q: start(back(2, *q))] for j, q in zip(main_steps, CHUNKS)}
    after[2] = [lambda q=q: relay_out(1, *q) for q in seconds]
    after[6].append(lambda: relay_reduce(3, 0))
    after[9].append(lambda: relay_reduce(3, 1))
    after[11].append(lambda: relay_reduce(3, 2))

    def work(i, carry):
        at(i, before)
        is_over = (i < 5) | (i == 8)

        @pl.when(is_over)
        def _():
            j = jnp.where(i == 8, 5, i)
            core, k = (s + j // COLORS) % 2, j % COLORS
            got = every[core, k].reshape(2 * TILE, dim)
            tail = note[core, k].reshape(2 * TILE, TAIL).astype(jnp.float32)
            flag_ref[...] = jnp.maximum(flag_ref[...], jnp.max(tail[:, COLORS:COLORS + 1], axis=0, keepdims=True))
            owner = jnp.sum(jnp.where(iota(tail.shape, 1) == k, tail, 0.0), axis=1, keepdims=True)
            result = expert_ffn(got, wg, wu, wd).astype(jnp.float32)
            result = jnp.where(owner == me, result, 0.0).astype(jnp.bfloat16)
            late[core, k] = result.reshape(SIDE, SIDE, SIDE, SPARE, dim)

        @pl.when(jnp.logical_not(is_over))
        def _():
            j = jnp.where(i < 8, i - 5, i - 6)
            k, sh = j % COLORS, (s + j // COLORS) % 2
            d[k, sh] = expert_ffn(d[k, sh].reshape(TILE, dim), wg, wu, wd).reshape(SIDE, SIDE, SIDE, PART, dim)

        at(i, after)
        return carry

    lax.fori_loop(0, 12, work, 0)
    for q in firsts:
        relay_back(2, *q)
    for k in range(COLORS):
        relay_reduce(4, k)
    for q in seconds:
        relay_back(2, *q)
    for k in range(COLORS):
        relay_reduce(2, k)
    for q in firsts:
        relay_back(1, *q)
    for k in range(COLORS):
        relay_reduce(1, k)
    for q in seconds:
        relay_back(1, *q)
    last[...] = jnp.zeros_like(last)
    for k in range(COLORS):
        relay_reduce(0, k)
    lanes = (iota((TILE, last.shape[0]), 1) + COLORS * rows).astype(jnp.float32)
    for part in range(tok // TILE):
        where = pl.ds(part * TILE, TILE)
        add = cols[where, 2:3] * dot(ones_where(cols[where, 0:1] == lanes), last[...])
        total[where, :] = add + cols[where, 3:4] * dot(ones_where(cols[where, 1:2] == lanes), last[...])

    def mix(i, final=False):
        k, sh = i % COLORS, (s + i // COLORS) % 2
        got = aa[k, sh].reshape(TILE, dim)
        lanes = (iota((TILE, TILE), 1) + (k * rows + sh * TILE)).astype(jnp.float32)
        for part in range(tok // TILE):
            where = pl.ds(part * TILE, TILE)
            add = cols[where, 2:3] * dot(ones_where(cols[where, 0:1] == lanes), got)
            add = add + cols[where, 3:4] * dot(ones_where(cols[where, 1:2] == lanes), got)
            if final:
                y_ref[where, :] = (total[where, :] + add).astype(jnp.bfloat16)
            else:
                total[where, :] += add

    def mix_early(i, carry):
        at(i, {j: [lambda q=q: drain(brought(0, *q), brecv.at[0, q[0], q[1]])] for j, q in enumerate(CHUNKS)})
        mix(i)
        return carry

    lax.fori_loop(0, len(CHUNKS) - 1, mix_early, 0)
    drain(brought(0, *CHUNKS[-1]), brecv.at[0, CHUNKS[-1][0], CHUNKS[-1][1]])
    mix(len(CHUNKS) - 1, final=True)
    for phase in range(3):
        for h in range(2):
            sent = d.at[:, 0] if phase == 0 and h else d.at[:, 0, 0:3]
            drain(sent, send.at[phase, h])
            drain(sent, bsend.at[phase, h])
    for phase in range(5):
        drain(gathered(every, slice(None))[phase], esend.at[phase])
        drain(gathered(note, 0)[phase], nsend.at[phase])
        drain((got1, got2, got3, stage, relay)[phase], rsend.at[phase])


def solution(mesh):
    n_sub, n_ep = mesh.shape["sub"], mesh.shape["ep"]
    n_dev = n_sub * n_ep
    tok_spec = P(("dp", "sub", "ep"), None)
    expert_spec = P(("sub", "ep"), None, None)
    group = ("sub", "ep")
    vmem = pl.BlockSpec(memory_space=pltpu.VMEM)
    hbm = pl.BlockSpec(memory_space=pl.ANY)
    params = pltpu.CompilerParams(vmem_limit_bytes=VMEM_LIMIT)
    bf16 = jnp.bfloat16

    def shape(*dims):
        return jax.ShapeDtypeStruct(dims, bf16)

    def weights(dim, ff):
        return [
            pl.BlockSpec((dim, ff), lambda i: (0, 0)),
            pl.BlockSpec((dim, ff), lambda i: (0, 0)),
            pl.BlockSpec((ff, dim), lambda i: (0, 0)),
        ]

    def wide(x, route, gate, w_gate, w_up, w_down):
        tok, dim = x.shape
        ff = w_gate.shape[1]
        cap = min(tok, 8 * tok // n_dev)
        rows = n_dev * cap
        send, pos = pl.pallas_call(
            functools.partial(wide_pack_kernel, cap),
            out_shape=[shape(rows, dim), jax.ShapeDtypeStruct((tok, 2), jnp.int32)],
            in_specs=[vmem, vmem],
            out_specs=[vmem, vmem],
            compiler_params=params,
            name="wide_pack",
        )(route, x)
        got = lax.all_to_all(send.reshape(n_dev, cap, dim), group, 0, 0).reshape(rows, dim)
        block = pl.BlockSpec((TILE, dim), lambda i: (i, 0))
        out = pl.pallas_call(
            wide_ffn_kernel,
            out_shape=shape(rows, dim),
            grid=(rows // TILE,),
            in_specs=[block] + weights(dim, ff),
            out_specs=block,
            compiler_params=params,
            name="wide_ffn",
        )(got, w_gate, w_up, w_down)
        ret = lax.all_to_all(out.reshape(n_dev, cap, dim), group, 0, 0).reshape(rows, dim)
        return pl.pallas_call(
            wide_mix_kernel,
            out_shape=shape(tok, dim),
            in_specs=[vmem, vmem, vmem],
            out_specs=vmem,
            compiler_params=params,
            name="wide_mix",
        )(ret, pos, gate)

    cube = (SIDE, SIDE, SIDE)

    def device_step(x, route, gate, w_gate, w_up, w_down):
        tok, dim = x.shape
        ff = w_gate.shape[2]
        w_gate, w_up, w_down = w_gate[0], w_up[0], w_down[0]
        sems = pltpu.SemaphoreType.DMA
        main = pltpu.VMEM((COLORS, 2) + cube + (PART, dim), bf16)
        one_way = sems((3, COLORS, 2))
        late_in, late_out = sems((5, COLORS)), sems((5,))
        y, flag = pl.pallas_call(
            layer_kernel,
            out_shape=[pltpu.VMEM((tok, dim), bf16), jax.ShapeDtypeStruct((1, 1), jnp.float32)],
            in_specs=[vmem, vmem, hbm, hbm, hbm, hbm],
            out_specs=[vmem, vmem],
            scratch_shapes=[
                pltpu.VMEM((tok, dim), bf16),
                pltpu.VMEM((dim, ff), bf16), pltpu.VMEM((dim, ff), bf16), pltpu.VMEM((ff, dim), bf16),
                main, main, main, main, main, main, main,
                pltpu.VMEM((2, COLORS) + cube + (SPARE, dim), bf16),
                pltpu.VMEM((2, COLORS) + cube + (SPARE, TAIL), bf16),
                pltpu.VMEM((2, COLORS) + cube + (SPARE, dim), bf16),
                pltpu.VMEM((COLORS,) + cube + (SPARE, dim), bf16),
                pltpu.VMEM((COLORS, SIDE, SIDE, SPARE, dim), bf16),
                pltpu.VMEM((COLORS, SIDE, SPARE, dim), bf16),
                pltpu.VMEM((COLORS, 2, SIDE // 2, SIDE, SPARE, dim), bf16),
                pltpu.VMEM((COLORS, 2, SIDE, SIDE, SPARE, dim), bf16),
                pltpu.VMEM((COLORS, SIDE - 1, SIDE, SPARE, dim), bf16),
                pltpu.VMEM((COLORS, SIDE - 1, SPARE, dim), bf16),
                pltpu.VMEM((128, dim), bf16),
                pltpu.VMEM((tok, 128), jnp.float32),
                pltpu.VMEM((tok, dim), jnp.float32),
                sems((3, 2)), one_way, sems((3, 2)), one_way, late_out, late_in, late_out, late_in, late_out, late_out, sems((4,)),
            ],
            compiler_params=pltpu.CompilerParams(
                collective_id=0, has_side_effects=True, vmem_limit_bytes=LAYER_VMEM),
            name="layer",
        )(route.T, gate.T, x, w_gate, w_up, w_down)
        return lax.cond(flag[0, 0] > 0.0, wide, lambda *args: y, x, route, gate, w_gate, w_up, w_down)

    return jax.shard_map(
        device_step,
        mesh=mesh,
        in_specs=(tok_spec, tok_spec, tok_spec, expert_spec, expert_spec, expert_spec),
        out_specs=tok_spec,
        check_vma=False,
    )
```
